256 devices in a mesh: dom: 256 (over y, z, x, core).
Axes of the slice: x: 4, y: 4, z: 8, core: 2. Of those that a mesh axis runs over, the one named last changes fastest.
Arguments:
- particles: bfloat16 [8192, 2, 7488], P('dom'), may hold values from -6 to 6
- references: bfloat16 [256, 2, 7488], P('dom'), may hold values from -6 to 6
- assignment: int32 [8192, 1], P('dom'), may hold values from 0 to 255
- orientation: int32 [8192], P('dom'), may hold values from 0 to 35
- tilt_range: int32 [2, 8192], P(None, 'dom'), may hold values from 0 to 20
Outputs:
- scores: float32 [8192, 256], P('dom')
- class_means: float32 [256, 2, 7488], P('dom')
- class_load: float32 [256], replicated
The draws below stay inside these ranges and needn't reach their ends.
Inputs may be any that keep to these rules, and one draw needn't show every extreme that they name: `assignment`: every class has at least one particle.
All inputs are finite; a program needn't handle non-finite values.
Results may differ from the reference program's by a relative error of at most 0.0035.
Values may be sent and summed in bfloat16 or wider, within the bound.
A program may use at most 128 MiB of HBM per device.

```python
import math
import jax
import jax.numpy as jnp
from jax import lax

GRID = 24
ORIENTS = 36
TILT_BINS = 21
PART_DEV = 32
CLASSES = 256
COEF = 7488
PARTICLES = 8192
N_DOM = 256


def with_ends(drawn, own_key, least, largest):
    place = [jax.random.randint(jax.random.fold_in(own_key, axis), (), 0, length) for axis, length in enumerate(drawn.shape)]
    widest = drawn.shape.index(max(drawn.shape))
    neighbour = place[:widest] + [(place[widest] + 1) % drawn.shape[widest]] + place[widest + 1:]
    return drawn.at[tuple(place)].set(least).at[tuple(neighbour)].set(largest)


def level_of(key, dims, cuts, low, largest):
    loudness = 1.0
    for axis_at, parts in cuts:
        draws = jax.random.uniform(jax.random.fold_in(jax.random.fold_in(key, 6), axis_at), (parts,), jnp.float32, low / len(cuts), largest / len(cuts))
        loudness = loudness * jnp.repeat(jnp.exp(draws), dims[axis_at] // parts).reshape((-1,) + (1,) * (len(dims) - 1 - axis_at))
    return loudness


def picks_of(rng, rows, number_of, top, lift):
    sequence = jax.random.permutation(jax.random.fold_in(rng, 1), number_of)
    boost = sequence
    for power in range(3):
        boost = boost * boost // number_of
    boost = boost * lift // number_of
    chance = jax.random.randint(jax.random.fold_in(rng, 2), (rows, number_of), 0, 4096) + boost
    holders = jax.random.permutation(jax.random.fold_in(rng, 3), rows)[jnp.arange(number_of) % rows]
    chance = jnp.where(jnp.arange(rows)[:, None] == holders[None, :], 1 << 14, chance)
    priority = chance * number_of + jnp.arange(number_of)
    return lax.top_k(priority.astype(jnp.int32), top)[1].astype(jnp.int32)


def noise(rng, shape, spread, most, pieces=(), kind=jnp.bfloat16):
    array = jax.random.normal(rng, shape, jnp.float32) * spread
    if len(pieces) > 0:
        array = level_of(rng, shape, pieces, -0.22, 0.18) * array
    return jnp.clip(array, min=-most, max=most).astype(kind)


def setup_inputs(seed: int = 0) -> dict:
    keys = jax.random.split(jax.random.key(seed), 6)
    return {
        "particles": noise(keys[0], (PARTICLES, 2, COEF), 1.0, 6.0, ((0, 256),)),
        "references": noise(keys[1], (CLASSES, 2, COEF), 1.0, 6.0, ((0, 256),)),
        "assignment": picks_of(keys[2], PARTICLES, CLASSES, 1, 32),
        "orientation": with_ends(jax.random.randint(keys[3], (PARTICLES,), 0, ORIENTS), jax.random.fold_in(keys[3], 1), 0, ORIENTS - 1).astype(jnp.int32),
        "tilt_range": with_ends(jax.random.randint(keys[4], (2, PARTICLES), 0, TILT_BINS), jax.random.fold_in(keys[4], 1), 0, TILT_BINS - 1).astype(jnp.int32),
    }


EPS = 1e-06
GAIN = 6.0
TAU = 0.5

def tables():
    index = jnp.arange(COEF, dtype=jnp.int32)
    plane = index // (GRID * GRID)
    rest = index % (GRID * GRID)
    col_x = rest // GRID
    col_z = rest % GRID
    freq_x = ((col_x + GRID // 2) % GRID - GRID // 2).astype(jnp.float32)
    freq_y = plane.astype(jnp.float32)
    freq_z = ((col_z + GRID // 2) % GRID - GRID // 2).astype(jnp.float32)
    return (freq_x, freq_y, freq_z)

def wedge_weights(orient, low_bin, high_bin):
    freq_x, freq_y, freq_z = tables()
    angle = orient.astype(jnp.float32) * (2.0 * math.pi / ORIENTS)
    along = -freq_x[None, :] * jnp.sin(angle)[:, None] + freq_y[None, :] * jnp.cos(angle)[:, None]
    radius = along * along + freq_z[None, :] * freq_z[None, :] + 1.0
    cos_two = (along * along - freq_z[None, :] * freq_z[None, :]) / radius
    sin_two = -2.0 * along * freq_z[None, :] / radius
    low = -(40.0 + 1.5 * low_bin.astype(jnp.float32)) * (math.pi / 180.0)
    high = (40.0 + 1.5 * high_bin.astype(jnp.float32)) * (math.pi / 180.0)
    centre = (low + high)[:, None]
    width = (high - low)[:, None]
    return jax.nn.sigmoid(GAIN * (cos_two * jnp.cos(centre) + sin_two * jnp.sin(centre) - jnp.cos(width)))

def reference(particles, references, assignment, orientation, tilt_range):
    ref32 = references.astype(jnp.float32)
    ref_power = (ref32[:, 0] * ref32[:, 0] + ref32[:, 1] * ref32[:, 1]).astype(jnp.bfloat16)
    ref_flat = references.reshape(CLASSES, 2 * COEF)
    part_blocks = particles.reshape(N_DOM, PART_DEV, 2, COEF)
    cls_blocks = assignment.reshape(N_DOM, PART_DEV)
    ori_blocks = orientation.reshape(N_DOM, PART_DEV)
    tilt_blocks = tilt_range.reshape(2, N_DOM, PART_DEV).transpose(1, 0, 2)
    class_ids = jnp.arange(CLASSES, dtype=jnp.int32)

    def step(carry, item):
        numer, denom, counts, totals = carry
        part, cls, ori, tilt = item
        wedge = wedge_weights(ori, tilt[0], tilt[1])
        pf = part.astype(jnp.float32)
        weighted = (wedge[:, None, :] * pf).astype(jnp.bfloat16)
        flat = weighted.reshape(PART_DEV, 2 * COEF)
        wedge_sq = (wedge * wedge).astype(jnp.bfloat16)
        wedge_low = wedge.astype(jnp.bfloat16)
        power = lax.optimization_barrier(jnp.sum(wedge * (pf[:, 0] * pf[:, 0] + pf[:, 1] * pf[:, 1]), axis=1))
        intersection = jnp.dot(flat, ref_flat.T, preferred_element_type=jnp.float32)
        energy = jnp.dot(wedge_low, ref_power.T, preferred_element_type=jnp.float32)
        scores = intersection / (math.sqrt(COEF) * jnp.sqrt((energy / COEF + EPS) * (power[:, None] / COEF + EPS)))
        onehot = (class_ids[:, None] == cls[None, :]).astype(jnp.bfloat16)
        numer = numer + jnp.dot(onehot, flat, preferred_element_type=jnp.float32)
        denom = denom + jnp.dot(onehot, wedge_sq, preferred_element_type=jnp.float32)
        onehot32 = onehot.astype(jnp.float32)
        counts = counts + lax.optimization_barrier(jnp.sum(onehot32, axis=1))
        totals = totals + jnp.dot(onehot32, lax.optimization_barrier(jnp.sum(wedge, axis=1)), precision=lax.Precision.HIGHEST)
        return ((numer, denom, counts, totals), scores)
    start = (jnp.zeros((CLASSES, 2 * COEF), jnp.float32), jnp.zeros((CLASSES, COEF), jnp.float32), jnp.zeros((CLASSES,), jnp.float32), jnp.zeros((CLASSES,), jnp.float32))
    (numer, denom, counts, totals), scores = lax.scan(step, start, (part_blocks, cls_blocks, ori_blocks, tilt_blocks))
    scores = scores.reshape(PARTICLES, CLASSES)
    bottom = denom + TAU * (totals[:, None] / COEF + 1.0)
    class_means = numer.reshape(CLASSES, 2, COEF) / bottom[:, None, :]
    class_load = counts * CLASSES / PARTICLES
    return (scores, class_means, class_load)
```

```python
import math

import jax
import jax.numpy as jnp
from jax import lax
from jax.experimental import pallas as pl
from jax.experimental.pallas import tpu as pltpu
from jax.sharding import Mesh
from jax.sharding import PartitionSpec as P

GRID = 24
ORIENTS = 36
COEF = 7488
CLASSES = 256
PARTICLES = 8192
EPS = 1e-06
GAIN = 6.0
TAU = 0.5

NY, NZ, NX, NC = 4, 8, 4, 2
NQ = NY * NX * NC
PART = 32
WIDE = 256
DOM = ("y", "z", "x", "c")
BF = jnp.bfloat16
F32 = jnp.float32


def frequencies(base, lanes=128):
    index = (lax.broadcasted_iota(jnp.int32, (1, lanes), 1) + base).astype(F32)
    plane = jnp.floor((index + 0.5) * (1.0 / (GRID * GRID)))
    rest = index - plane * (GRID * GRID)
    col_x = jnp.floor((rest + 0.5) * (1.0 / GRID))
    col_z = rest - col_x * GRID
    half = GRID // 2
    freq_x = jnp.where(col_x < half, col_x, col_x - GRID)
    freq_z = jnp.where(col_z < half, col_z, col_z - GRID)
    square_z = freq_z * freq_z
    return freq_x, plane, square_z, square_z + 1.0, -2.0 * freq_z, index


def wedge_of(feature, freq):
    sine, cosine, cos_centre, sin_centre, cos_width = feature
    freq_x, freq_y, square_z, square_z1, minus_2z, _ = freq
    along = freq_y * cosine - freq_x * sine
    square = along * along
    turned = ((square - square_z) * cos_centre + (minus_2z * along) * sin_centre) / (square + square_z1)
    return 1.0 / (1.0 + jnp.exp(-GAIN * (turned - cos_width)))


def kernel(
    feat_ref, ref_ref, x_ref,
    score_ref, mean_ref, count_ref,
    fb, r0, xb, stb, c_dummy,
    r1, rr, nb, nr, db, dr, st, zs, s8, tcol,
    pad0, pad1, ft0, ft1, oh, wg, wlow, wsq, wx, rf, rpow,
    sbi, sbe, pbi, pbe, sm, b1, mb,
    f_s, f_r, a_s, a_r, x_s, x_r, t_s, t_r, m_s, m_r,
    rz_s, rz_r, dz_s, dz_r, nz_s, nz_r, sz_s, sz_r,
    pe_s, pe_r, pi_s, pi_r, b_s, b_r,
):
    y = lax.axis_index("y")
    z = lax.axis_index("z")
    x = lax.axis_index("x")
    c = lax.axis_index("c")
    q = y * 8 + x * 2 + c
    chip = y * 4 + x

    def at_plane(t):
        return {"y": t // 8, "z": z, "x": (t // 2) % 4, "c": t % 2}

    def at_z(t):
        return {"y": y, "z": t, "x": x, "c": c}

    def at_chip(t):
        return {"y": t // 4, "z": z, "x": t % 4, "c": c}

    other = {"y": y, "z": z, "x": x, "c": 1 - c}

    def exchange(size, me, place, src, dst, send, recv):
        def copy(t, s):
            return pltpu.make_async_remote_copy(
                src_ref=src(t), dst_ref=dst(s), send_sem=send.at[t], recv_sem=recv.at[s],
                device_id=place(t), device_id_type=pl.DeviceIdType.MESH,
            )

        def start():
            def one(d, _):
                copy((me + d) % size, me).start()
                return 0

            lax.fori_loop(1, size, one, 0)

        def wait_one(d):
            s = (me + size - d) % size
            copy(s, s).wait_recv()
            return s

        def wait_recv():
            def one(d, _):
                wait_one(d)
                return 0

            lax.fori_loop(1, size, one, 0)

        def wait_send():
            def one(d, _):
                copy((me + d) % size, me).wait_send()
                return 0

            lax.fori_loop(1, size, one, 0)

        return start, wait_recv, wait_send, wait_one

    barrier = pltpu.get_barrier_semaphore()

    def greet(d, _):
        pl.semaphore_signal(
            barrier, inc=1, device_id=at_plane((q + d) % NQ), device_id_type=pl.DeviceIdType.MESH
        )
        return 0

    def greet_z(d, _):
        pl.semaphore_signal(
            barrier, inc=1, device_id=at_z((z + d) % NZ), device_id_type=pl.DeviceIdType.MESH
        )
        return 0

    lax.fori_loop(1, NQ, greet, 0)
    lax.fori_loop(1, NZ, greet_z, 0)
    pl.semaphore_wait(barrier, NQ - 1 + NZ - 1)

    feats = exchange(NQ, q, at_plane, lambda t: feat_ref, lambda s: fb.at[s], f_s, f_r)
    refs0 = exchange(NQ, q, at_plane, lambda t: ref_ref.at[t], lambda s: r0.at[s], a_s, a_r)
    parts = exchange(NQ, q, at_plane, lambda t: x_ref.at[t], lambda s: xb.at[s], x_s, x_r)
    stats = exchange(NQ, q, at_plane, lambda t: st, lambda s: stb.at[s], t_s, t_r)
    means = exchange(NQ, q, at_plane, lambda t: mb.at[t], lambda s: mean_ref.at[s], m_s, m_r)
    refsz = exchange(NZ, z, at_z, lambda t: r1, lambda s: rr.at[s], rz_s, rz_r)

    def rows32(t):
        return pl.ds(pl.multiple_of(t * 32, 32), 32)

    denz = exchange(NZ, z, at_z, lambda t: db.at[rows32(t)], lambda s: dr.at[s], dz_s, dz_r)
    numz = exchange(NZ, z, at_z, lambda t: nb.at[:, rows32(t)], lambda s: nr.at[s], nz_s, nz_r)
    statz = exchange(NZ, z, at_z, lambda t: s8, lambda s: zs.at[s], sz_s, sz_r)
    backs = exchange(16, chip, at_chip, lambda t: sm.at[t], lambda s: b1.at[s], b_s, b_r)

    def to_other(src, dst, send, recv):
        return pltpu.make_async_remote_copy(
            src_ref=src.at[:, 1 - c], dst_ref=dst, send_sem=send, recv_sem=recv,
            device_id=other, device_id_type=pl.DeviceIdType.MESH,
        )

    swap_e = to_other(sbe, pbe, pe_s, pe_r)
    swap_i = to_other(sbi, pbi, pi_s, pi_r)

    feats[0]()
    refs0[0]()
    parts[0]()

    fb[pl.ds(q, 1)] = feat_ref[...][None]
    r0[pl.ds(q, 1)] = ref_ref[pl.ds(q, 1)]
    xb[pl.ds(q, 1)] = x_ref[pl.ds(q, 1)]
    pad0[...] = jnp.zeros_like(pad0)
    pad1[...] = jnp.zeros_like(pad1)

    feats[1]()
    pad0[0:32, :] = fb[:, 0, :]
    pad1[0:32, :] = fb[:, 1, :]
    ft0[...] = pad0[...].T
    ft1[...] = pad1[...].T
    class_row = lax.broadcasted_iota(jnp.int32, (CLASSES, 128), 0).astype(F32)
    for tile in range(8):
        row = jnp.sum(fb[4 * tile : 4 * tile + 4, 2, :], axis=0, keepdims=True)
        oh[:, tile * 128 : tile * 128 + 128] = jnp.where(class_row == row, 1.0, 0.0).astype(BF)

    def column(ft, block, lane):
        return jnp.take_along_axis(ft[block * 32 : block * 32 + 32, :], lane, axis=1, mode="promise_in_bounds")

    def features(s):
        lane = jnp.full((32, 128), s, jnp.int32)
        return tuple(column(ft0, k, lane) for k in range(4)) + (column(ft1, 0, lane),)

    mine = [frequencies(q * WIDE), frequencies(q * WIDE + 128)]

    def weigh(s, _):
        feature = features(s)
        for half in range(2):
            wedge = wedge_of(feature, mine[half])
            where = (rows32(s), slice(half * 128, half * 128 + 128))
            wg[where] = wedge
            wlow[where] = wedge.astype(BF)
            wsq[where] = (wedge * wedge).astype(BF)
        return 0

    lax.fori_loop(0, NQ, weigh, 0)

    refs0[1]()
    for part in range(2):
        r1[part] = r0[:, part, :].astype(BF)
    refsz[0]()
    rr[pl.ds(z, 1)] = r1[...][None]

    db[...] = jnp.dot(oh[...], wsq[...], preferred_element_type=F32).astype(BF)
    denz[0]()
    dr[pl.ds(z, 1)] = db[rows32(z)][None]

    own = features(q)

    def own_slice(s, carry):
        power, total = carry
        for half in range(2):
            freq = frequencies(s * WIDE + half * 128)
            wedge = wedge_of(own, freq)
            real = x_ref[s, 0:32, half * 128 : half * 128 + 128].astype(F32)
            imag = x_ref[s, 32:64, half * 128 : half * 128 + 128].astype(F32)
            power = power + wedge * (real * real + imag * imag)
            total = total + jnp.where(freq[5] < COEF, wedge, 0.0)
        return power, total

    nothing = jnp.zeros((32, 128), F32)
    power, total = lax.fori_loop(0, NQ, own_slice, (nothing, nothing))
    power = jnp.sum(power, axis=1, keepdims=True)
    total = jnp.sum(total, axis=1, keepdims=True)
    own_class = column(ft1, 2, jnp.full((32, 128), q, jnp.int32))
    for half in range(2):
        ids = (lax.broadcasted_iota(jnp.int32, (32, 128), 1) + half * 128).astype(F32)
        hit = own_class == ids
        lanes = slice(half * 128, half * 128 + 128)
        st[0:1, lanes] = jnp.sum(jnp.where(hit, 1.0, 0.0), axis=0, keepdims=True)
        st[1:2, lanes] = jnp.sum(jnp.where(hit, total, 0.0), axis=0, keepdims=True)
    stats[0]()
    stb[pl.ds(q, 1)] = st[...][None]

    refsz[1]()
    for part in range(2):
        for plane in range(NZ):
            block = rr[plane, part].astype(F32)
            for k in range(NY):
                rf[part, k * 64 + plane * 8 : k * 64 + plane * 8 + 8, :] = block[8 * k : 8 * k + 8]
    rpow[...] = (rf[0] * rf[0] + rf[1] * rf[1]).astype(BF)
    contract = (((1,), (1,)), ((), ()))
    sbe[...] = lax.dot_general(wlow[...], rpow[...], contract, preferred_element_type=F32).reshape(16, 2, 32, CLASSES)
    swap_e.start()

    def weight(s):
        for part in range(2):
            value = xb[s, 32 * part : 32 * part + 32, :].astype(F32)
            wx[part, rows32(s), :] = (wg[rows32(s), :] * value).astype(BF)

    weight(q)

    def arrive(d, _):
        weight(parts[3](d))
        return 0

    lax.fori_loop(1, NQ, arrive, 0)
    for part in range(2):
        nb[part] = jnp.dot(oh[...], wx[part], preferred_element_type=F32).astype(BF)
    numz[0]()
    nr[pl.ds(z, 1)] = nb[:, rows32(z)][None]

    inter = lax.dot_general(wx[0], rf[0].astype(BF), contract, preferred_element_type=F32)
    inter = inter + lax.dot_general(wx[1], rf[1].astype(BF), contract, preferred_element_type=F32)
    sbi[...] = inter.reshape(16, 2, 32, CLASSES)
    swap_i.start()
    swap_e.wait_recv()
    swap_i.wait_recv()

    def add_core(t, _):
        sm[t, 0] = (sbi[t, c] + pbi[t]).astype(BF)
        sm[t, 1] = (sbe[t, c] + pbe[t]).astype(BF)
        return 0

    lax.fori_loop(0, 16, add_core, 0)
    backs[0]()
    b1[pl.ds(chip, 1)] = sm[pl.ds(chip, 1)]

    stats[1]()
    s8[...] = jnp.sum(stb[...], axis=0)
    statz[0]()
    zs[pl.ds(z, 1)] = s8[...][None]
    statz[1]()
    every = jnp.sum(zs[...], axis=0)
    count_ref[...] = every * (CLASSES / PARTICLES)
    tcol[...] = jnp.zeros_like(tcol)
    tcol[0:2, :] = every
    turned = [tcol[:, 0:128].T, tcol[:, 128:256].T]
    pad0[...] = turned[0]
    pad1[...] = turned[1]

    denz[1]()
    numz[1]()
    denom = jnp.sum(dr[...].astype(F32), axis=0)
    tail = jnp.concatenate(
        [(pad0, pad1)[k // 2][pl.ds(pl.multiple_of((k % 2) * 64 + z * 8, 8), 8), 1:2] for k in range(NY)], axis=0
    )
    bottom = denom + TAU * (tail / COEF + 1.0)
    for part in range(2):
        top = jnp.sum(nr[:, part].astype(F32), axis=0)
        mb[:, part, :] = top / bottom
    means[0]()
    mean_ref[pl.ds(q, 1)] = mb[pl.ds(q, 1)]

    backs[1]()
    inter = jnp.sum(b1[:, 0].astype(F32), axis=0)
    energy = jnp.sum(b1[:, 1].astype(F32), axis=0)
    score_ref[...] = inter / (
        math.sqrt(COEF) * jnp.sqrt((energy / COEF + EPS) * (power / COEF + EPS))
    )
    means[1]()
    for group in (feats, refs0, parts, stats, means, refsz, denz, numz, statz, backs):
        group[2]()
    swap_e.wait_send()
    swap_i.wait_send()


def body(particles, references, assignment, orientation, tilt_range):
    q = lax.axis_index("y") * 8 + lax.axis_index("x") * 2 + lax.axis_index("c")
    padded = NQ * WIDE
    cls = assignment[:, 0]
    angle = orientation.astype(F32) * (2.0 * math.pi / ORIENTS)
    low = -(40.0 + 1.5 * tilt_range[0].astype(F32)) * (math.pi / 180.0)
    high = (40.0 + 1.5 * tilt_range[1].astype(F32)) * (math.pi / 180.0)
    nil = jnp.zeros((PART,), F32)
    in_plane = ((cls // 8) % 8 * 32 + cls // 64 * 8 + cls % 8).astype(F32)
    spot = (jnp.arange(4) == q % 4).astype(F32)
    feat = jnp.stack(
        [
            jnp.concatenate([jnp.sin(angle), jnp.cos(angle), jnp.cos(low + high), jnp.sin(low + high)]),
            jnp.concatenate([jnp.cos(high - low), in_plane, cls.astype(F32), nil]),
            (spot[:, None] * in_plane[None, :]).reshape(128),
            jnp.zeros((128,), F32),
        ]
    )
    refs = jnp.pad(references[0].astype(F32), ((0, 0), (0, padded - COEF)))
    refs = refs.reshape(2, NQ, WIDE).transpose(1, 0, 2)
    xs = jnp.pad(particles, ((0, 0), (0, 0), (0, padded - COEF)))
    xs = xs.reshape(PART, 2, NQ, WIDE).transpose(2, 1, 0, 3).reshape(NQ, 2 * PART, WIDE)

    def v(*shape, dtype=F32):
        return pltpu.VMEM(shape, dtype)

    sem = pltpu.SemaphoreType.DMA
    vm = pl.BlockSpec(memory_space=pltpu.VMEM)
    scores, means, counts = pl.pallas_call(
        kernel,
        out_shape=(
            jax.ShapeDtypeStruct((PART, CLASSES), F32),
            jax.ShapeDtypeStruct((NQ, 2, WIDE), F32),
            jax.ShapeDtypeStruct((2, CLASSES), F32),
        ),
        in_specs=[vm] * 3,
        out_specs=(vm,) * 3,
        scratch_shapes=[
            v(NQ, 4, 128), v(NQ, 2, WIDE), v(NQ, 64, WIDE, dtype=BF), v(NQ, 2, CLASSES), v(8, 128),
            v(2, 32, WIDE, dtype=BF), v(NZ, 2, 32, WIDE, dtype=BF),
            v(2, CLASSES, WIDE, dtype=BF), v(NZ, 2, 32, WIDE, dtype=BF),
            v(CLASSES, WIDE, dtype=BF), v(NZ, 32, WIDE, dtype=BF),
            v(2, CLASSES), v(NZ, 2, CLASSES), v(2, CLASSES), v(128, CLASSES),
            v(128, 128), v(128, 128), v(128, 128), v(128, 128),
            v(CLASSES, 1024, dtype=BF), v(1024, WIDE), v(1024, WIDE, dtype=BF), v(1024, WIDE, dtype=BF),
            v(2, 1024, WIDE, dtype=BF), v(2, CLASSES, WIDE), v(CLASSES, WIDE, dtype=BF),
            v(16, 2, 32, CLASSES), v(16, 2, 32, CLASSES), v(16, 32, CLASSES), v(16, 32, CLASSES),
            v(16, 2, 32, CLASSES, dtype=BF), v(16, 2, 32, CLASSES, dtype=BF), v(NQ, 2, WIDE),
        ] + [sem((NQ,))] * 10 + [sem((NZ,))] * 8 + [sem] * 4 + [sem((16,))] * 2,
        compiler_params=pltpu.CompilerParams(
            collective_id=0, has_side_effects=True, vmem_limit_bytes=48 * 2**20
        ),
    )(feat, refs, xs)
    class_means = means.transpose(1, 0, 2).reshape(1, 2, padded)[:, :, :COEF]
    return scores, class_means, counts[0]


def solution(mesh):
    split = Mesh(mesh.devices.reshape(NY, NZ, NX, NC), DOM)
    placed = (P(DOM, None, None), P(DOM, None, None), P(DOM, None), P(DOM), P(None, DOM))
    return jax.shard_map(
        body,
        mesh=split,
        in_specs=placed,
        out_specs=(P(DOM, None), P(DOM, None, None), P()),
        check_vma=False,
    )
```

```python
import math

import jax
import jax.numpy as jnp
from jax import lax
from jax.experimental import pallas as pl
from jax.experimental.pallas import tpu as pltpu
from jax.sharding import Mesh
from jax.sharding import PartitionSpec as P

GRID = 24
ORIENTS = 36
COEF = 7488
CLASSES = 256
PARTICLES = 8192
EPS = 1e-06
GAIN = 6.0
TAU = 0.5

NY, NZ, NX, NC = 4, 8, 4, 2
NQ = NY * NX * NC
PART = 32
WIDE = 256
DOM = ("y", "z", "x", "c")
BF = jnp.bfloat16
F32 = jnp.float32


def frequencies(base, lanes=128):
    index = (lax.broadcasted_iota(jnp.int32, (1, lanes), 1) + base).astype(F32)
    plane = jnp.floor((index + 0.5) * (1.0 / (GRID * GRID)))
    rest = index - plane * (GRID * GRID)
    col_x = jnp.floor((rest + 0.5) * (1.0 / GRID))
    col_z = rest - col_x * GRID
    half = GRID // 2
    freq_x = jnp.where(col_x < half, col_x, col_x - GRID)
    freq_z = jnp.where(col_z < half, col_z, col_z - GRID)
    square_z = freq_z * freq_z
    return freq_x, plane, square_z, square_z + 1.0, -2.0 * freq_z, index


def wedge_of(feature, freq):
    sine, cosine, cos_centre, sin_centre, cos_width = feature
    freq_x, freq_y, square_z, square_z1, minus_2z, _ = freq
    along = freq_y * cosine - freq_x * sine
    square = along * along
    turned = ((square - square_z) * cos_centre + (minus_2z * along) * sin_centre) / (square + square_z1)
    return 1.0 / (1.0 + jnp.exp(-GAIN * (turned - cos_width)))


def kernel(
    part_hbm, ref_hbm, cls_hbm, ori_hbm, tilt_hbm,
    score_ref, mean_ref, count_ref,
    raw, rawr, lab_c, lab_o, lab_t, cm, cb, xs, xb, st, stb,
    r1, rr, nb, nr, db, dr, s8, zs, tcol,
    pad0, pad1, ft0, ft1, oh, wg, wlow, wsq, wx, rf, rpow,
    sbi, sbe, pbi, pbe, sm, b1, mb,
    in_s, lab_s, c_s, c_r, x_s, x_r, t_s, t_r, m_s, m_r,
    rz_s, rz_r, dz_s, dz_r, nz_s, nz_r, sz_s, sz_r,
    pe_s, pe_r, pi_s, pi_r, b_s, b_r,
):
    y = lax.axis_index("y")
    z = lax.axis_index("z")
    x = lax.axis_index("x")
    c = lax.axis_index("c")
    q = y * 8 + x * 2 + c
    chip = y * 4 + x

    def at_plane(t):
        return {"y": t // 8, "z": z, "x": (t // 2) % 4, "c": t % 2}

    def at_z(t):
        return {"y": y, "z": t, "x": x, "c": c}

    def at_chip(t):
        return {"y": t // 4, "z": z, "x": t % 4, "c": c}

    other = {"y": y, "z": z, "x": x, "c": 1 - c}

    def over(first, last, step):
        def one(d, _):
            step(d)
            return 0

        lax.fori_loop(first, last, one, 0)

    def exchange(size, me, place, src, dst, blocks, send, recv):
        def start_one(d):
            t = (me + d) % size
            pltpu.make_async_remote_copy(
                src_ref=src(t), dst_ref=dst(me), send_sem=send, recv_sem=recv,
                device_id=place(t), device_id_type=pl.DeviceIdType.MESH,
            ).start()

        def start():
            over(1, size, start_one)

        def wait_recv():
            pltpu.make_async_copy(blocks, blocks, recv).wait()

        def wait_send():
            pltpu.make_async_copy(blocks, blocks, send).wait()

        return start, wait_recv, wait_send

    def rows32(t):
        return pl.ds(pl.multiple_of(t * 32, 32), 32)

    reads = [
        pltpu.make_async_copy(part_hbm, raw, in_s.at[0]),
        pltpu.make_async_copy(ref_hbm, rawr, in_s.at[1]),
        pltpu.make_async_copy(cls_hbm, lab_c, lab_s.at[0]),
        pltpu.make_async_copy(ori_hbm, lab_o, lab_s.at[1]),
        pltpu.make_async_copy(tilt_hbm, lab_t, lab_s.at[2]),
    ]
    for read in reads:
        read.start()

    barrier = pltpu.get_barrier_semaphore()

    def greet(place, me, size):
        def one(d):
            pl.semaphore_signal(
                barrier, inc=1, device_id=place((me + d) % size), device_id_type=pl.DeviceIdType.MESH
            )

        over(1, size, one)

    greet(at_plane, q, NQ)
    greet(at_z, z, NZ)

    few = pl.ds(0, NQ - 1)
    fewz = pl.ds(0, NZ - 1)
    mixed = exchange(NQ, q, at_plane, lambda t: cm.at[t], lambda s: cb.at[s], cb.at[few], c_s, c_r)
    parts = exchange(NQ, q, at_plane, lambda t: xs.at[t], lambda s: xb.at[s], xb.at[few], x_s, x_r)
    stats = exchange(NQ, q, at_plane, lambda t: st, lambda s: stb.at[s], stb.at[few], t_s, t_r)
    means = exchange(NQ, q, at_plane, lambda t: mb.at[t], lambda s: mean_ref.at[s], mb.at[few], m_s, m_r)
    refsz = exchange(NZ, z, at_z, lambda t: r1, lambda s: rr.at[s], rr.at[fewz], rz_s, rz_r)
    denz = exchange(NZ, z, at_z, lambda t: db.at[rows32(t)], lambda s: dr.at[s], dr.at[fewz], dz_s, dz_r)
    numz = exchange(NZ, z, at_z, lambda t: nb.at[:, rows32(t)], lambda s: nr.at[s], nr.at[fewz], nz_s, nz_r)
    statz = exchange(NZ, z, at_z, lambda t: s8, lambda s: zs.at[s], zs.at[fewz], sz_s, sz_r)
    backs = exchange(16, chip, at_chip, lambda t: sm.at[t], lambda s: b1.at[s], b1.at[pl.ds(0, 15)], b_s, b_r)

    def to_other(src, dst, send, recv):
        return pltpu.make_async_remote_copy(
            src_ref=src.at[:, 1 - c], dst_ref=dst, send_sem=send, recv_sem=recv,
            device_id=other, device_id_type=pl.DeviceIdType.MESH,
        )

    swap_e = to_other(sbe, pbe, pe_s, pe_r)
    swap_i = to_other(sbi, pbi, pi_s, pi_r)

    for read in reads[2:]:
        read.wait()
    lane = lax.broadcasted_iota(jnp.int32, (1, 128), 1)
    cls = lab_c[...]
    in_plane = (((cls >> 3) & 7) * 32 + (cls >> 6) * 8 + (cls & 7)).astype(F32)
    angle = lab_o[...].astype(F32) * (2.0 * math.pi / ORIENTS)
    low = -(40.0 + 1.5 * lab_t[0:1, :].astype(F32)) * (math.pi / 180.0)
    high = (40.0 + 1.5 * lab_t[1:2, :].astype(F32)) * (math.pi / 180.0)
    packed = jnp.concatenate([angle, angle, low + high, low + high], axis=1)
    row0 = jnp.where((lane < 32) | (lane >= 96), jnp.sin(packed), jnp.cos(packed))
    row1 = jnp.concatenate([jnp.cos(high - low), in_plane, cls.astype(F32), jnp.zeros((1, 32), F32)], axis=1)
    row2 = jnp.where(lane // 32 == q % 4, jnp.concatenate([in_plane] * 4, axis=1), 0.0)
    cm[:, 2:3, 0:128] = jnp.broadcast_to(row0[None], (NQ, 1, 128))
    cm[:, 2:3, 128:256] = jnp.broadcast_to(row1[None], (NQ, 1, 128))
    cm[:, 3:4, 0:128] = jnp.broadcast_to(row2[None], (NQ, 1, 128))
    cm[:, 3:4, 128:256] = jnp.zeros((NQ, 1, 128), F32)
    reads[1].wait()
    whole = COEF // WIDE
    rest = COEF - whole * WIDE
    for t in range(NQ):
        if t < whole:
            cm[t, 0:2, :] = rawr[0, :, t * WIDE : (t + 1) * WIDE].astype(F32)
        else:
            cm[t, 0:2, :] = jnp.zeros((2, WIDE), F32)
    cm[whole, 0:2, 0:rest] = rawr[0, :, whole * WIDE : COEF].astype(F32)

    reads[0].wait()

    def relay(t):
        block = raw[:, :, pl.ds(pl.multiple_of(t * WIDE, WIDE), WIDE)]
        xs[t] = jnp.swapaxes(block, 0, 1).reshape(2 * PART, WIDE)

    over(0, whole, relay)
    for t in range(whole, NQ):
        xs[t] = jnp.zeros((2 * PART, WIDE), BF)
    xs[whole, :, 0:rest] = jnp.swapaxes(raw[:, :, whole * WIDE : COEF], 0, 1).reshape(2 * PART, rest)
    pl.semaphore_wait(barrier, NQ - 1 + NZ - 1)

    mixed[0]()
    parts[0]()
    cb[pl.ds(q, 1)] = cm[pl.ds(q, 1)]
    xb[pl.ds(q, 1)] = xs[pl.ds(q, 1)]

    def column(ft, block, index):
        return jnp.take_along_axis(ft[block * 32 : block * 32 + 32, :], index, axis=1, mode="promise_in_bounds")

    def features(s):
        index = jnp.full((32, 128), s, jnp.int32)
        return tuple(column(ft0, k, index) for k in range(4)) + (column(ft1, 0, index),)

    pad0[...] = jnp.broadcast_to(row0, (128, 128))
    pad1[...] = jnp.broadcast_to(row1, (128, 128))
    ft0[...] = pad0[...].T
    ft1[...] = pad1[...].T
    own = tuple(ft0[k * 32 : k * 32 + 32, :] for k in range(4)) + (ft1[0:32, :],)
    own_class = ft1[64:96, :]

    def own_slice(s, carry):
        power, total = carry
        for half in range(2):
            freq = frequencies(s * WIDE + half * 128)
            wedge = wedge_of(own, freq)
            real = xs[s, 0:32, half * 128 : half * 128 + 128].astype(F32)
            imag = xs[s, 32:64, half * 128 : half * 128 + 128].astype(F32)
            power = power + wedge * (real * real + imag * imag)
            total = total + jnp.where(freq[5] < COEF, wedge, 0.0)
        return power, total

    nothing = jnp.zeros((32, 128), F32)
    power, total = lax.fori_loop(0, NQ, own_slice, (nothing, nothing))
    power = jnp.sum(power, axis=1, keepdims=True)
    total = jnp.sum(total, axis=1, keepdims=True)
    for half in range(2):
        ids = (lax.broadcasted_iota(jnp.int32, (32, 128), 1) + half * 128).astype(F32)
        hit = own_class == ids
        lanes = slice(half * 128, half * 128 + 128)
        st[0:1, lanes] = jnp.sum(jnp.where(hit, 1.0, 0.0), axis=0, keepdims=True)
        st[1:2, lanes] = jnp.sum(jnp.where(hit, total, 0.0), axis=0, keepdims=True)
    stats[0]()
    stb[pl.ds(q, 1)] = st[...][None]

    mixed[1]()
    for part in range(2):
        r1[part] = cb[:, part, :].astype(BF)
    refsz[0]()
    rr[pl.ds(z, 1)] = r1[...][None]

    pad0[0:32, :] = cb[:, 2, 0:128]
    pad1[0:32, :] = cb[:, 2, 128:256]
    ft0[...] = pad0[...].T
    ft1[...] = pad1[...].T
    class_row = lax.broadcasted_iota(jnp.int32, (CLASSES, 128), 0).astype(F32)
    for tile in range(8):
        row = jnp.sum(cb[4 * tile : 4 * tile + 4, 3, 0:128], axis=0, keepdims=True)
        oh[:, tile * 128 : tile * 128 + 128] = jnp.where(class_row == row, 1.0, 0.0).astype(BF)

    mine = [frequencies(q * WIDE), frequencies(q * WIDE + 128)]

    def weigh(s):
        feature = features(s)
        for half in range(2):
            wedge = wedge_of(feature, mine[half])
            where = (rows32(s), slice(half * 128, half * 128 + 128))
            wg[where] = wedge
            wlow[where] = wedge.astype(BF)
            wsq[where] = (wedge * wedge).astype(BF)

    over(0, NQ, weigh)

    db[...] = jnp.dot(oh[...], wsq[...], preferred_element_type=F32).astype(BF)
    denz[0]()
    dr[pl.ds(z, 1)] = db[rows32(z)][None]

    refsz[1]()
    for part in range(2):
        for plane in range(NZ):
            block = rr[plane, part].astype(F32)
            for k in range(NY):
                rf[part, k * 64 + plane * 8 : k * 64 + plane * 8 + 8, :] = block[8 * k : 8 * k + 8]
    rpow[...] = (rf[0] * rf[0] + rf[1] * rf[1]).astype(BF)
    contract = (((1,), (1,)), ((), ()))
    sbe[...] = lax.dot_general(wlow[...], rpow[...], contract, preferred_element_type=F32).reshape(16, 2, 32, CLASSES)
    swap_e.start()

    parts[1]()
    stats[1]()
    s8[...] = jnp.sum(stb[...], axis=0)
    statz[0]()
    zs[pl.ds(z, 1)] = s8[...][None]

    def weight(s):
        for part in range(2):
            value = xb[s, 32 * part : 32 * part + 32, :].astype(F32)
            wx[part, rows32(s), :] = (wg[rows32(s), :] * value).astype(BF)

    over(0, NQ, weight)
    inter = lax.dot_general(wx[0], rf[0].astype(BF), contract, preferred_element_type=F32)
    inter = inter + lax.dot_general(wx[1], rf[1].astype(BF), contract, preferred_element_type=F32)
    sbi[...] = inter.reshape(16, 2, 32, CLASSES)
    swap_i.start()
    for part in range(2):
        nb[part] = jnp.dot(oh[...], wx[part], preferred_element_type=F32).astype(BF)
    numz[0]()
    nr[pl.ds(z, 1)] = nb[:, rows32(z)][None]

    swap_e.wait_recv()
    swap_i.wait_recv()

    def add_core(t):
        sm[t, 0] = (sbi[t, c] + pbi[t]).astype(BF)
        sm[t, 1] = (sbe[t, c] + pbe[t]).astype(BF)

    over(0, 16, add_core)
    backs[0]()
    b1[pl.ds(chip, 1)] = sm[pl.ds(chip, 1)]

    statz[1]()
    every = jnp.sum(zs[...], axis=0)
    count_ref[...] = every * (CLASSES / PARTICLES)
    tcol[...] = jnp.zeros_like(tcol)
    tcol[0:2, :] = every
    turned = [tcol[:, 0:128].T, tcol[:, 128:256].T]
    pad0[...] = turned[0]
    pad1[...] = turned[1]

    denz[1]()
    denom = jnp.sum(dr[...].astype(F32), axis=0)
    tail = jnp.concatenate(
        [(pad0, pad1)[k // 2][pl.ds(pl.multiple_of((k % 2) * 64 + z * 8, 8), 8), 1:2] for k in range(NY)], axis=0
    )
    bottom = denom + TAU * (tail / COEF + 1.0)
    numz[1]()
    for part in range(2):
        top = jnp.sum(nr[:, part].astype(F32), axis=0)
        mb[:, part, :] = top / bottom
    means[0]()
    mean_ref[pl.ds(q, 1)] = mb[pl.ds(q, 1)]

    backs[1]()
    inter = jnp.sum(b1[:, 0].astype(F32), axis=0)
    energy = jnp.sum(b1[:, 1].astype(F32), axis=0)
    score_ref[...] = inter / (
        math.sqrt(COEF) * jnp.sqrt((energy / COEF + EPS) * (power / COEF + EPS))
    )
    means[1]()
    for group in (mixed, parts, stats, means, refsz, denz, numz, statz, backs):
        group[2]()
    swap_e.wait_send()
    swap_i.wait_send()


def body(particles, references, assignment, orientation, tilt_range):
    padded = NQ * WIDE

    def v(*shape, dtype=F32):
        return pltpu.VMEM(shape, dtype)

    sem = pltpu.SemaphoreType.DMA
    vm = pl.BlockSpec(memory_space=pltpu.VMEM)
    anywhere = pl.BlockSpec(memory_space=pl.ANY)
    scores, means, counts = pl.pallas_call(
        kernel,
        out_shape=(
            jax.ShapeDtypeStruct((PART, CLASSES), F32),
            jax.ShapeDtypeStruct((NQ, 2, WIDE), F32),
            jax.ShapeDtypeStruct((2, CLASSES), F32),
        ),
        in_specs=[anywhere] * 5,
        out_specs=(vm,) * 3,
        scratch_shapes=[
            v(PART, 2, COEF, dtype=BF), v(1, 2, COEF, dtype=BF),
            v(1, PART, dtype=jnp.int32), v(1, PART, dtype=jnp.int32), v(2, PART, dtype=jnp.int32),
            v(NQ, 4, WIDE), v(NQ, 4, WIDE), v(NQ, 64, WIDE, dtype=BF), v(NQ, 64, WIDE, dtype=BF),
            v(2, CLASSES), v(NQ, 2, CLASSES),
            v(2, 32, WIDE, dtype=BF), v(NZ, 2, 32, WIDE, dtype=BF),
            v(2, CLASSES, WIDE, dtype=BF), v(NZ, 2, 32, WIDE, dtype=BF),
            v(CLASSES, WIDE, dtype=BF), v(NZ, 32, WIDE, dtype=BF),
            v(2, CLASSES), v(NZ, 2, CLASSES), v(128, CLASSES),
            v(128, 128), v(128, 128), v(128, 128), v(128, 128),
            v(CLASSES, 1024, dtype=BF), v(1024, WIDE), v(1024, WIDE, dtype=BF), v(1024, WIDE, dtype=BF),
            v(2, 1024, WIDE, dtype=BF), v(2, CLASSES, WIDE), v(CLASSES, WIDE, dtype=BF),
            v(16, 2, 32, CLASSES), v(16, 2, 32, CLASSES), v(16, 32, CLASSES), v(16, 32, CLASSES),
            v(16, 2, 32, CLASSES, dtype=BF), v(16, 2, 32, CLASSES, dtype=BF), v(NQ, 2, WIDE),
            sem((2,)), sem((3,)),
        ] + [sem] * 22,
        compiler_params=pltpu.CompilerParams(
            collective_id=0, has_side_effects=True, vmem_limit_bytes=48 * 2**20
        ),
    )(particles, references, assignment.T, orientation[None], tilt_range)
    class_means = means.transpose(1, 0, 2).reshape(1, 2, padded)[:, :, :COEF]
    return scores, class_means, counts[0]


def solution(mesh):
    split = Mesh(mesh.devices.reshape(NY, NZ, NX, NC), DOM)
    placed = (P(DOM, None, None), P(DOM, None, None), P(DOM, None), P(DOM), P(None, DOM))
    return jax.shard_map(
        body,
        mesh=split,
        in_specs=placed,
        out_specs=(P(DOM, None), P(DOM, None, None), P()),
        check_vma=False,
    )
```

```python
import math

import jax
import jax.numpy as jnp
from jax import lax
from jax.experimental import pallas as pl
from jax.experimental.pallas import tpu as pltpu
from jax.sharding import Mesh
from jax.sharding import PartitionSpec as P

GRID = 24
ORIENTS = 36
COEF = 7488
CLASSES = 256
PARTICLES = 8192
EPS = 1e-06
GAIN = 6.0
TAU = 0.5

NY, NZ, NX, NC = 4, 8, 4, 2
NQ = NY * NX * NC
PART = 32
WIDE = 256
DOM = ("y", "z", "x", "c")
BF = jnp.bfloat16
F32 = jnp.float32


def frequencies(base, lanes=128):
    index = (lax.broadcasted_iota(jnp.int32, (1, lanes), 1) + base).astype(F32)
    plane = jnp.floor((index + 0.5) * (1.0 / (GRID * GRID)))
    rest = index - plane * (GRID * GRID)
    col_x = jnp.floor((rest + 0.5) * (1.0 / GRID))
    col_z = rest - col_x * GRID
    half = GRID // 2
    freq_x = jnp.where(col_x < half, col_x, col_x - GRID)
    freq_z = jnp.where(col_z < half, col_z, col_z - GRID)
    square_z = freq_z * freq_z
    return freq_x, plane, square_z, square_z + 1.0, -2.0 * freq_z, index


def wedge_of(feature, freq):
    sine, cosine, cos_centre, sin_centre, cos_width = feature
    freq_x, freq_y, square_z, square_z1, minus_2z, _ = freq
    along = freq_y * cosine - freq_x * sine
    square = along * along
    turned = ((square - square_z) * cos_centre + (minus_2z * along) * sin_centre) / (square + square_z1)
    return 1.0 / (1.0 + jnp.exp(-GAIN * (turned - cos_width)))


def kernel(
    part_hbm, ref_hbm, cls_hbm, ori_hbm, tilt_hbm,
    score_ref, mean_ref, count_ref,
    raw, rawr, lab_c, lab_o, lab_t, cm, cb, xs, xb, st, stb,
    r1, rr, nb, nr, db, dr, s8, zs, tcol,
    pad0, pad1, ft, sel, oh, wg, wlow, wsq, wx, rf, rpow,
    sbi, sbe, pbi, pbe, sm, b1, mb, mr,
    in_s, lab_s, x_s, x_r, nz_s, nz_r, c_s, c_r, t_s, t_r, m_s, m_r,
    rz_s, rz_r, dz_s, dz_r, sz_s, sz_r,
    pe_s, pe_r, pi_s, pi_r, b_s, b_r,
):
    y = lax.axis_index("y")
    z = lax.axis_index("z")
    x = lax.axis_index("x")
    c = lax.axis_index("c")
    q = y * 8 + x * 2 + c
    chip = y * 4 + x

    def at_plane(t):
        return {"y": t // 8, "z": z, "x": (t // 2) % 4, "c": t % 2}

    def at_z(t):
        return {"y": y, "z": t, "x": x, "c": c}

    def at_chip(t):
        return {"y": t // 4, "z": z, "x": t % 4, "c": c}

    other = {"y": y, "z": z, "x": x, "c": 1 - c}

    def over(first, last, step):
        def one(d, _):
            step(d)
            return 0

        lax.fori_loop(first, last, one, 0)

    def exchange(size, me, place, src, dst, blocks, send, recv):
        def start_one(d):
            t = (me + d) % size
            pltpu.make_async_remote_copy(
                src_ref=src(t), dst_ref=dst(me), send_sem=send, recv_sem=recv,
                device_id=place(t), device_id_type=pl.DeviceIdType.MESH,
            ).start()

        def start():
            over(1, size, start_one)

        def wait_recv():
            pltpu.make_async_copy(blocks, blocks, recv).wait()

        def wait_send():
            pltpu.make_async_copy(blocks, blocks, send).wait()

        return start, wait_recv, wait_send

    def rows32(t):
        return pl.ds(pl.multiple_of(t * 32, 32), 32)

    barrier = pltpu.get_barrier_semaphore()

    def greet(place, me, size):
        def one(d):
            pl.semaphore_signal(
                barrier, inc=1, device_id=place((me + d) % size), device_id_type=pl.DeviceIdType.MESH
            )

        over(1, size, one)

    greet(at_plane, q, NQ)
    greet(at_z, z, NZ)

    reads = [
        pltpu.make_async_copy(part_hbm, raw, in_s.at[0]),
        pltpu.make_async_copy(ref_hbm, rawr, in_s.at[1]),
        pltpu.make_async_copy(cls_hbm, lab_c, lab_s.at[0]),
        pltpu.make_async_copy(ori_hbm, lab_o, lab_s.at[1]),
        pltpu.make_async_copy(tilt_hbm, lab_t, lab_s.at[2]),
    ]
    for read in reads:
        read.start()

    few = pl.ds(0, NQ - 1)
    fewz = pl.ds(0, NZ - 1)
    mixed = exchange(NQ, q, at_plane, lambda t: cm.at[t], lambda s: cb.at[s], cb.at[few], c_s, c_r)

    def parts_of(h):
        return exchange(
            NQ, q, at_plane, lambda t: xs.at[h, t], lambda s: xb.at[h, s], xb.at[h, few], x_s.at[h], x_r.at[h]
        )

    parts = [parts_of(0), parts_of(1)]
    stats = exchange(NQ, q, at_plane, lambda t: st, lambda s: stb.at[s], stb.at[few], t_s, t_r)
    means = exchange(NQ, q, at_plane, lambda t: mb.at[t], lambda s: mr.at[s], mr.at[few], m_s, m_r)
    refsz = exchange(NZ, z, at_z, lambda t: r1, lambda s: rr.at[s], rr.at[fewz], rz_s, rz_r)
    denz = exchange(NZ, z, at_z, lambda t: db.at[rows32(t)], lambda s: dr.at[s], dr.at[fewz], dz_s, dz_r)

    def numz_of(h):
        return exchange(
            NZ, z, at_z, lambda t: nb.at[h, rows32(t)], lambda s: nr.at[h, s], nr.at[h, fewz], nz_s.at[h], nz_r.at[h]
        )

    numz = [numz_of(0), numz_of(1)]
    statz = exchange(NZ, z, at_z, lambda t: s8, lambda s: zs.at[s], zs.at[fewz], sz_s, sz_r)
    backs = exchange(16, chip, at_chip, lambda t: sm.at[t], lambda s: b1.at[s], b1.at[pl.ds(0, 15)], b_s, b_r)

    def to_other(src, dst, send, recv):
        return pltpu.make_async_remote_copy(
            src_ref=src.at[:, 1 - c], dst_ref=dst, send_sem=send, recv_sem=recv,
            device_id=other, device_id_type=pl.DeviceIdType.MESH,
        )

    swap_e = to_other(sbe, pbe, pe_s, pe_r)
    swap_i = to_other(sbi, pbi, pi_s, pi_r)

    for read in reads[2:]:
        read.wait()
    labels = jnp.concatenate([lab_c[...], lab_o[...], lab_t[0:1, :], lab_t[1:2, :]], axis=1).astype(F32)
    pair = jnp.concatenate([labels, jnp.zeros((1, 128), F32)], axis=0).astype(BF)
    cm[:, 2:4, 0:128] = jnp.broadcast_to(pair[None], (NQ, 2, 128))
    cm[:, 2:4, 128:256] = jnp.zeros((NQ, 2, 128), BF)
    reads[1].wait()
    whole = COEF // WIDE
    rest = COEF - whole * WIDE
    for t in range(NQ):
        if t < whole:
            cm[t, 0:2, :] = rawr[0, :, t * WIDE : (t + 1) * WIDE]
        else:
            cm[t, 0:2, :] = jnp.zeros((2, WIDE), BF)
    cm[whole, 0:2, 0:rest] = rawr[0, :, whole * WIDE : COEF]

    reads[0].wait()

    def relay(t):
        for h in range(2):
            block = raw[:, :, pl.ds(pl.multiple_of(t * WIDE + h * 128, 128), 128)]
            both = jnp.swapaxes(block, 0, 1)
            xs[h, t, :, 0:128] = both[0]
            xs[h, t, :, 128:256] = both[1]

    over(0, whole, relay)
    for h in range(2):
        for t in range(whole, NQ):
            xs[h, t] = jnp.zeros((PART, WIDE), BF)
    both = jnp.swapaxes(raw[:, :, whole * WIDE : COEF], 0, 1)
    xs[0, whole, :, 0:rest] = both[0]
    xs[0, whole, :, 128 : 128 + rest] = both[1]
    pl.semaphore_wait(barrier, NQ - 1 + NZ - 1)

    mixed[0]()
    parts[0][0]()
    parts[1][0]()
    cb[pl.ds(q, 1)] = cm[pl.ds(q, 1)]
    for h in range(2):
        xb[h, pl.ds(q, 1)] = xs[h, pl.ds(q, 1)]

    def features_of(turned):
        angle = turned[32:64] * (2.0 * math.pi / ORIENTS)
        low = -(40.0 + 1.5 * turned[64:96]) * (math.pi / 180.0)
        high = (40.0 + 1.5 * turned[96:128]) * (math.pi / 180.0)
        centre = low + high
        return jnp.sin(angle), jnp.cos(angle), jnp.cos(centre), jnp.sin(centre), jnp.cos(high - low)

    pad0[...] = jnp.broadcast_to(labels, (128, 128))
    turned = pad0[...].T
    own = features_of(turned)
    own_class = turned[0:32]

    def own_slice(s, carry):
        power, total = carry
        for half in range(2):
            freq = frequencies(s * WIDE + half * 128)
            wedge = wedge_of(own, freq)
            real = xs[half, s, :, 0:128].astype(F32)
            imag = xs[half, s, :, 128:256].astype(F32)
            power = power + wedge * (real * real + imag * imag)
            total = total + jnp.where(freq[5] < COEF, wedge, 0.0)
        return power, total

    nothing = jnp.zeros((32, 128), F32)
    power, total = lax.fori_loop(0, NQ, own_slice, (nothing, nothing))
    power = jnp.sum(power, axis=1, keepdims=True)
    total = jnp.sum(total, axis=1, keepdims=True)
    for half in range(2):
        ids = (lax.broadcasted_iota(jnp.int32, (32, 128), 1) + half * 128).astype(F32)
        hit = own_class == ids
        lanes = slice(half * 128, half * 128 + 128)
        st[0:1, lanes] = jnp.sum(jnp.where(hit, 1.0, 0.0), axis=0, keepdims=True)
        st[1:2, lanes] = jnp.sum(jnp.where(hit, total, 0.0), axis=0, keepdims=True)
    stats[0]()
    stb[pl.ds(q, 1)] = st[...][None]

    mixed[1]()
    both = jnp.swapaxes(cb[:, 0:2, :], 0, 1)
    for h in range(2):
        for part in range(2):
            at = h * 256 + part * 128
            r1[:, at : at + 128] = both[part, :, h * 128 : h * 128 + 128]
    refsz[0]()
    rr[pl.ds(z, 1)] = r1[...][None]

    every = jnp.swapaxes(cb[:, 2:4, 0:128], 0, 1)[0].astype(F32)
    pad0[0:32, :] = every
    for k, feature in enumerate(features_of(pad0[...].T)):
        ft[k] = feature
    sub = lax.broadcasted_iota(jnp.int32, (32, 128), 0)
    cls = jnp.where(lax.broadcasted_iota(jnp.int32, (32, 128), 1) < 32, every, 0.0).astype(jnp.int32)
    in_plane = (((cls >> 3) & 7) * 32 + (cls >> 6) * 8 + (cls & 7)).astype(F32)
    chosen = in_plane
    for k in range(1, 4):
        chosen = jnp.where((sub & 3) == k, pltpu.roll(in_plane, 32 * k, 1), chosen)
    sel[...] = chosen
    class_row = lax.broadcasted_iota(jnp.int32, (CLASSES, 128), 0).astype(F32)
    for tile in range(8):
        row = jnp.sum(sel[4 * tile : 4 * tile + 4, :], axis=0, keepdims=True)
        oh[:, tile * 128 : tile * 128 + 128] = jnp.where(class_row == row, 1.0, 0.0).astype(BF)

    def features(s):
        index = jnp.full((32, 128), s, jnp.int32)
        return tuple(jnp.take_along_axis(ft[k], index, axis=1, mode="promise_in_bounds") for k in range(5))

    mine = [frequencies(q * WIDE), frequencies(q * WIDE + 128)]

    def weigh(s):
        feature = features(s)
        for half in range(2):
            wedge = wedge_of(feature, mine[half])
            where = (rows32(s), slice(half * 128, half * 128 + 128))
            wg[where] = wedge
            wlow[where] = wedge.astype(BF)
            wsq[where] = (wedge * wedge).astype(BF)

    over(0, NQ, weigh)

    db[...] = jnp.dot(oh[...], wsq[...], preferred_element_type=F32).astype(BF)
    denz[0]()
    dr[pl.ds(z, 1)] = db[rows32(z)][None]

    def half_sums(h):
        def weight(s):
            wedge = wg[rows32(s), h * 128 : h * 128 + 128]
            block = xb[h, s].astype(F32)
            wx[h, rows32(s), 0:128] = (wedge * block[:, 0:128]).astype(BF)
            wx[h, rows32(s), 128:256] = (wedge * block[:, 128:256]).astype(BF)

        over(0, NQ, weight)
        nb[h] = jnp.dot(oh[...], wx[h], preferred_element_type=F32).astype(BF)
        numz[h][0]()
        nr[h, pl.ds(z, 1)] = nb[h, rows32(z)][None]

    parts[0][1]()
    half_sums(0)

    refsz[1]()
    for plane in range(NZ):
        block = rr[plane].astype(F32)
        for k in range(NY):
            rf[k * 64 + plane * 8 : k * 64 + plane * 8 + 8, :] = block[8 * k : 8 * k + 8]
    for h in range(2):
        real = rf[:, h * 256 : h * 256 + 128]
        imag = rf[:, h * 256 + 128 : h * 256 + 256]
        rpow[:, h * 128 : h * 128 + 128] = (real * real + imag * imag).astype(BF)
    contract = (((1,), (1,)), ((), ()))
    sbe[...] = lax.dot_general(wlow[...], rpow[...], contract, preferred_element_type=F32).reshape(16, 2, 32, CLASSES)
    swap_e.start()
    part_sum = lax.dot_general(wx[0], rf[:, 0:256].astype(BF), contract, preferred_element_type=F32)
    sbi[...] = part_sum.reshape(16, 2, 32, CLASSES)

    parts[1][1]()
    half_sums(1)
    part_sum = lax.dot_general(wx[1], rf[:, 256:512].astype(BF), contract, preferred_element_type=F32)
    sbi[...] += part_sum.reshape(16, 2, 32, CLASSES)
    swap_i.start()

    stats[1]()
    s8[...] = jnp.sum(stb[...], axis=0)
    statz[0]()
    zs[pl.ds(z, 1)] = s8[...][None]

    swap_e.wait_recv()
    swap_i.wait_recv()

    def add_core(t):
        sm[t, 0] = (sbi[t, c] + pbi[t]).astype(BF)
        sm[t, 1] = (sbe[t, c] + pbe[t]).astype(BF)

    over(0, 16, add_core)
    backs[0]()
    b1[pl.ds(chip, 1)] = sm[pl.ds(chip, 1)]

    statz[1]()
    every = jnp.sum(zs[...], axis=0)
    count_ref[...] = every[0:1] * (CLASSES / PARTICLES)
    tcol[...] = jnp.zeros_like(tcol)
    tcol[0:2, :] = every
    pad0[...] = tcol[:, 0:128].T
    pad1[...] = tcol[:, 128:256].T

    denz[1]()
    denom = jnp.sum(dr[...].astype(F32), axis=0)
    tail = jnp.concatenate(
        [(pad0, pad1)[k // 2][pl.ds(pl.multiple_of((k % 2) * 64 + z * 8, 8), 8), 1:2] for k in range(NY)], axis=0
    )
    bottom = denom + TAU * (tail / COEF + 1.0)
    scale = 1.0 / bottom
    for h in range(2):
        numz[h][1]()
        top = jnp.sum(nr[h].astype(F32), axis=0)
        for part in range(2):
            lanes = slice(h * 128, h * 128 + 128)
            mb[:, part, lanes] = top[:, part * 128 : part * 128 + 128] * scale[:, lanes]
    means[0]()
    mr[pl.ds(q, 1)] = mb[pl.ds(q, 1)]

    backs[1]()
    inter = jnp.sum(b1[:, 0].astype(F32), axis=0)
    energy = jnp.sum(b1[:, 1].astype(F32), axis=0)
    score_ref[...] = inter / (
        math.sqrt(COEF) * jnp.sqrt((energy / COEF + EPS) * (power / COEF + EPS))
    )
    means[1]()
    for t in range(whole):
        mean_ref[0, :, t * WIDE : (t + 1) * WIDE] = mr[t]
    mean_ref[0, :, whole * WIDE : COEF] = mr[whole, :, 0:rest]
    for group in (mixed, *parts, stats, means, refsz, denz, *numz, statz, backs):
        group[2]()
    swap_e.wait_send()
    swap_i.wait_send()


def leave(score_in, mean_in, count_in, score_ref, mean_ref, count_ref, send):
    copies = [
        pltpu.make_async_copy(score_in, score_ref, send.at[0]),
        pltpu.make_async_copy(mean_in, mean_ref, send.at[1]),
        pltpu.make_async_copy(count_in, count_ref, send.at[2]),
    ]
    for copy in copies:
        copy.start()
    for copy in copies:
        copy.wait()


def body(particles, references, assignment, orientation, tilt_range):
    def v(*shape, dtype=F32):
        return pltpu.VMEM(shape, dtype)

    sem = pltpu.SemaphoreType.DMA
    vm = pl.BlockSpec(memory_space=pltpu.VMEM)
    hbm = pl.BlockSpec(memory_space=pltpu.HBM)
    shapes = (
        jax.ShapeDtypeStruct((PART, CLASSES), F32),
        jax.ShapeDtypeStruct((1, 2, COEF), F32),
        jax.ShapeDtypeStruct((1, CLASSES), F32),
    )
    outs = pl.pallas_call(
        kernel,
        out_shape=shapes,
        in_specs=[hbm] * 5,
        out_specs=(vm,) * 3,
        scratch_shapes=[
            v(PART, 2, COEF, dtype=BF), v(1, 2, COEF, dtype=BF),
            v(1, PART, dtype=jnp.int32), v(1, PART, dtype=jnp.int32), v(2, PART, dtype=jnp.int32),
            v(NQ, 4, WIDE, dtype=BF), v(NQ, 4, WIDE, dtype=BF),
            v(2, NQ, PART, WIDE, dtype=BF), v(2, NQ, PART, WIDE, dtype=BF),
            v(2, CLASSES), v(NQ, 2, CLASSES),
            v(32, 2 * WIDE, dtype=BF), v(NZ, 32, 2 * WIDE, dtype=BF),
            v(2, CLASSES, WIDE, dtype=BF), v(2, NZ, 32, WIDE, dtype=BF),
            v(CLASSES, WIDE, dtype=BF), v(NZ, 32, WIDE, dtype=BF),
            v(2, CLASSES), v(NZ, 2, CLASSES), v(128, CLASSES),
            v(128, 128), v(128, 128), v(5, 32, 128), v(32, 128),
            v(CLASSES, 1024, dtype=BF), v(1024, WIDE), v(1024, WIDE, dtype=BF), v(1024, WIDE, dtype=BF),
            v(2, 1024, WIDE, dtype=BF), v(CLASSES, 2 * WIDE), v(CLASSES, WIDE, dtype=BF),
            v(16, 2, 32, CLASSES), v(16, 2, 32, CLASSES), v(16, 32, CLASSES), v(16, 32, CLASSES),
            v(16, 2, 32, CLASSES, dtype=BF), v(16, 2, 32, CLASSES, dtype=BF), v(NQ, 2, WIDE), v(NQ, 2, WIDE),
        ] + [sem((2,)), sem((3,))] + [sem((2,))] * 4 + [sem] * 18,
        compiler_params=pltpu.CompilerParams(
            collective_id=0, has_side_effects=True
        ),
    )(particles, references, assignment.T, orientation[None], tilt_range)
    scores, means, counts = pl.pallas_call(
        leave, out_shape=shapes, in_specs=[vm] * 3, out_specs=(hbm,) * 3, scratch_shapes=[sem((3,))]
    )(*outs)
    return scores, means, counts[0]


def solution(mesh):
    split = Mesh(mesh.devices.reshape(NY, NZ, NX, NC), DOM)
    placed = (P(DOM, None, None), P(DOM, None, None), P(DOM, None), P(DOM), P(None, DOM))
    return jax.shard_map(
        body,
        mesh=split,
        in_specs=placed,
        out_specs=(P(DOM, None), P(DOM, None, None), P()),
        check_vma=False,
    )
```

```python
import math

import jax
import jax.numpy as jnp
from jax import lax
from jax.experimental import pallas as pl
from jax.experimental.pallas import tpu as pltpu
from jax.sharding import Mesh
from jax.sharding import PartitionSpec as P

GRID = 24
ORIENTS = 36
COEF = 7488
CLASSES = 256
PARTICLES = 8192
EPS = 1e-06
GAIN = 6.0
TAU = 0.5

NY, NZ, NX, NC = 4, 8, 4, 2
NQ = NY * NX * NC
PART = 32
WIDE = 256
TILE = 128
AROUND = (
    (2, 2), (1, 2), (3, 2), (2, 1), (2, 3), (0, 2), (2, 0),
    (1, 1), (3, 3), (1, 3), (3, 1), (0, 1), (0, 3), (1, 0), (3, 0),
)
SINGLE = (5, 12, 19, 26, 31)
DOM = ("y", "z", "x", "c")
BF = jnp.bfloat16
F32 = jnp.float32


def first_tile(q):
    return 2 * q - (q + 1) // 7


def frequencies(base, lanes=128):
    index = (lax.broadcasted_iota(jnp.int32, (1, lanes), 1) + base).astype(F32)
    plane = jnp.floor((index + 0.5) * (1.0 / (GRID * GRID)))
    rest = index - plane * (GRID * GRID)
    col_x = jnp.floor((rest + 0.5) * (1.0 / GRID))
    col_z = rest - col_x * GRID
    half = GRID // 2
    freq_x = jnp.where(col_x < half, col_x, col_x - GRID)
    freq_z = jnp.where(col_z < half, col_z, col_z - GRID)
    square_z = freq_z * freq_z
    return freq_x, plane, square_z, square_z + 1.0, -2.0 * freq_z, index


def wedge_of(feature, freq):
    sine, cosine, cos_centre, sin_centre, cos_width = feature
    freq_x, freq_y, square_z, square_z1, minus_2z, _ = freq
    along = freq_y * cosine - freq_x * sine
    square = along * along
    turned = ((square - square_z) * cos_centre + (minus_2z * along) * sin_centre) / (square + square_z1)
    return 1.0 / (1.0 + jnp.exp(-GAIN * (turned - cos_width)))


def kernel(
    part_hbm, ref_hbm, cls_hbm, ori_hbm, tilt_hbm,
    score_ref, mean_ref, count_ref,
    raw, rawr, lab_c, lab_o, lab_t, cm, cb, xs, xb, tm, tmr,
    r1, rr, nb, nr, db, dr, s8, zs,
    pad0, ft, sel, oh, wg, wlow, wsq, wx, rf, rpow,
    sbi, sbe, pbi, pbe, sm, b1, mb, mr,
    in_s, lab_s, x_s, x_r, nz_s, nz_r, b_s, b_r, c_s, c_r, t_s, t_r, m_s, m_r,
    rz_s, rz_r, dz_s, dz_r, sz_s, sz_r,
    pe_s, pe_r, pi_s, pi_r,
):
    y = lax.axis_index("y")
    z = lax.axis_index("z")
    x = lax.axis_index("x")
    c = lax.axis_index("c")
    q = y * 8 + x * 2 + c
    chip = y * 4 + x

    def to_chip(dy, dx, dc):
        ty, tx, tc = (y + dy) & 3, (x + dx) & 3, c ^ dc
        return (ty * 8 + tx * 2 + tc, ty * 4 + tx), {"y": ty, "z": z, "x": tx, "c": tc}

    def plane_peers():
        for dy, dx in AROUND:
            for dc in (0, 1):
                yield lambda dy=dy, dx=dx, dc=dc: to_chip(dy, dx, dc)
        yield lambda: to_chip(0, 0, 1)

    def chip_peers():
        for dy, dx in AROUND:
            yield lambda dy=dy, dx=dx: to_chip(dy, dx, 0)

    def z_peers():
        for d in (4, 3, 5, 2, 6, 1, 7):

            def peer(d=d):
                t = (z + d) & 7
                return (t, t), {"y": y, "z": t, "x": x, "c": c}

            yield peer

    other = {"y": y, "z": z, "x": x, "c": 1 - c}

    def over(first, last, step, unroll=1):
        def one(d, _):
            step(d)
            return 0

        lax.fori_loop(first, last, one, 0, unroll=unroll)

    def pair(t):
        return (t % 7 != 5) & (t != 31)

    def exchange(group, me, src, dst, blocks, send, recv, wants=None):
        peers, index = {"plane": (plane_peers, 0), "chip": (chip_peers, 1), "z": (z_peers, 0)}[group]

        def start():
            for peer in peers():
                ts, place = peer()
                t = ts[index]
                copy = pltpu.make_async_remote_copy(
                    src_ref=src(t), dst_ref=dst(me), send_sem=send, recv_sem=recv,
                    device_id=place, device_id_type=pl.DeviceIdType.MESH,
                )
                if wants is None:
                    copy.start()
                else:
                    pl.when(wants(t))(copy.start)

        def wait_recv():
            pltpu.make_async_copy(blocks, blocks, recv).wait()

        def wait_send():
            pltpu.make_async_copy(blocks, blocks, send).wait()

        return start, wait_recv, wait_send

    def rows32(t):
        return pl.ds(pl.multiple_of(t * 32, 32), 32)

    reads = [
        pltpu.make_async_copy(part_hbm, raw, in_s.at[0]),
        pltpu.make_async_copy(ref_hbm, rawr, in_s.at[1]),
        pltpu.make_async_copy(cls_hbm, lab_c, lab_s.at[0]),
        pltpu.make_async_copy(ori_hbm, lab_o, lab_s.at[1]),
        pltpu.make_async_copy(tilt_hbm, lab_t, lab_s.at[2]),
    ]
    for read in reads:
        read.start()

    barrier = pltpu.get_barrier_semaphore()

    for peers in (plane_peers, z_peers):
        for peer in peers():
            pl.semaphore_signal(barrier, inc=1, device_id=peer()[1], device_id_type=pl.DeviceIdType.MESH)

    few = pl.ds(0, NQ - 1)
    fewz = pl.ds(0, NZ - 1)
    mixed = exchange("plane", q, lambda t: cm.at[t], lambda s: cb.at[s], cb.at[few], c_s, c_r)

    def parts_of(h):
        return exchange(
            "plane", q, lambda t: xs.at[h, t], lambda s: xb.at[h, s], xb.at[h, few], x_s.at[h], x_r.at[h],
            pair if h else None,
        )

    parts = [parts_of(0), parts_of(1)]
    double = pair(q)

    def second_arrived():
        @pl.when(double)
        def _():
            parts[1][1]()

    def second_sent():
        for case, others in ((double, NQ - len(SINGLE) - 1), (jnp.logical_not(double), NQ - len(SINGLE))):

            @pl.when(case)
            def _():
                sent = xb.at[1, pl.ds(0, others)]
                pltpu.make_async_copy(sent, sent, x_s.at[1]).wait()

    totals = exchange("plane", q, lambda t: tm, lambda s: tmr.at[s], tmr.at[few], t_s, t_r)
    means = exchange("plane", q, lambda t: mb.at[t], lambda s: mr.at[s], mr.at[few], m_s, m_r)
    refsz = exchange("z", z, lambda t: r1, lambda s: rr.at[s], rr.at[fewz], rz_s, rz_r)
    denz = exchange("z", z, lambda t: db.at[rows32(t)], lambda s: dr.at[s], dr.at[fewz], dz_s, dz_r)

    def numz_of(h):
        return exchange(
            "z", z, lambda t: nb.at[h, rows32(t)], lambda s: nr.at[h, s], nr.at[h, fewz], nz_s.at[h], nz_r.at[h]
        )

    numz = [numz_of(0), numz_of(1)]
    statz = exchange("z", z, lambda t: s8, lambda s: zs.at[s], zs.at[fewz], sz_s, sz_r)

    def backs_of(k):
        return exchange(
            "chip", chip, lambda t: sm.at[k, t], lambda s: b1.at[k, s], b1.at[k, pl.ds(0, 15)], b_s.at[k], b_r.at[k]
        )

    backs = [backs_of(0), backs_of(1)]

    def to_other(src, dst, send, recv):
        return pltpu.make_async_remote_copy(
            src_ref=src.at[:, 1 - c], dst_ref=dst, send_sem=send, recv_sem=recv,
            device_id=other, device_id_type=pl.DeviceIdType.MESH,
        )

    swap_e = to_other(sbe, pbe, pe_s, pe_r)
    swap_i = to_other(sbi, pbi, pi_s, pi_r)

    for read in reads[2:]:
        read.wait()
    labels = jnp.concatenate([lab_c[...], lab_o[...], lab_t[0:1, :], lab_t[1:2, :]], axis=1).astype(F32)
    two_rows = jnp.concatenate([labels, jnp.zeros((1, 128), F32)], axis=0).astype(BF)
    cm[:, 2:4, 0:128] = jnp.broadcast_to(two_rows[None], (NQ, 2, 128))
    cm[:, 2:4, 128:256] = jnp.zeros((NQ, 2, 128), BF)
    reads[1].wait()
    for t in range(NQ):
        first = first_tile(t) * TILE
        size = min(TILE if t in SINGLE else WIDE, COEF - first)
        if size < WIDE:
            cm[t, 0:2, :] = jnp.zeros((2, WIDE), BF)
        cm[t, 0:2, 0:size] = rawr[0, :, first : first + size]

    reads[0].wait()

    for t in range(NQ):
        first = first_tile(t) * TILE
        size = min(TILE if t in SINGLE else WIDE, COEF - first)
        both = jnp.swapaxes(raw[:, :, first : first + size], 0, 1)
        for h in range(2):
            wide = min(TILE, size - h * TILE)
            if wide < TILE:
                xs[h, t] = jnp.zeros((PART, WIDE), BF)
            if wide > 0:
                for part in range(2):
                    xs[h, t, :, part * TILE : part * TILE + wide] = both[part, :, h * TILE : h * TILE + wide]
    pl.semaphore_wait(barrier, NQ - 1 + NZ - 1)

    mixed[0]()
    parts[0][0]()
    parts[1][0]()
    cb[pl.ds(q, 1)] = cm[pl.ds(q, 1)]

    @pl.when(jnp.logical_not(double))
    def _():
        xb[1] = jnp.zeros((NQ, PART, WIDE), BF)

    for h in range(2):
        xb[h, pl.ds(q, 1)] = xs[h, pl.ds(q, 1)]

    def features_of(turned):
        angle = turned[32:64] * (2.0 * math.pi / ORIENTS)
        low = -(40.0 + 1.5 * turned[64:96]) * (math.pi / 180.0)
        high = (40.0 + 1.5 * turned[96:128]) * (math.pi / 180.0)
        centre = low + high
        return jnp.sin(angle), jnp.cos(angle), jnp.cos(centre), jnp.sin(centre), jnp.cos(high - low)

    pad0[...] = jnp.broadcast_to(labels, (128, 128))
    own = features_of(pad0[...].T)

    def own_slice(s, power):
        for half in range(2):
            wedge = wedge_of(own, frequencies((first_tile(s) + half) * TILE))
            real = xs[half, s, :, 0:128].astype(F32)
            imag = xs[half, s, :, 128:256].astype(F32)
            power = power + wedge * (real * real + imag * imag)
        return power

    power = lax.fori_loop(0, NQ, own_slice, jnp.zeros((32, 128), F32), unroll=2)
    power = jnp.sum(power, axis=1, keepdims=True)

    mixed[1]()
    both = jnp.swapaxes(cb[:, 0:2, :], 0, 1)
    for h in range(2):
        for part in range(2):
            at = h * 256 + part * 128
            r1[:, at : at + 128] = both[part, :, h * 128 : h * 128 + 128]
    refsz[0]()
    rr[pl.ds(z, 1)] = r1[...][None]

    every = jnp.swapaxes(cb[:, 2:4, 0:128], 0, 1)[0].astype(F32)
    pad0[0:32, :] = every
    for k, feature in enumerate(features_of(pad0[...].T)):
        ft[k] = feature
    sub = lax.broadcasted_iota(jnp.int32, (32, 128), 0)
    cls = jnp.where(lax.broadcasted_iota(jnp.int32, (32, 128), 1) < 32, every, 0.0).astype(jnp.int32)
    in_plane = (((cls >> 3) & 7) * 32 + (cls >> 6) * 8 + (cls & 7)).astype(F32)
    chosen = in_plane
    for k in range(1, 4):
        chosen = jnp.where((sub & 3) == k, pltpu.roll(in_plane, 32 * k, 1), chosen)
    sel[...] = chosen
    class_row = lax.broadcasted_iota(jnp.int32, (CLASSES, 128), 0).astype(F32)
    for tile in range(8):
        row = jnp.sum(sel[4 * tile : 4 * tile + 4, :], axis=0, keepdims=True)
        oh[:, tile * 128 : tile * 128 + 128] = jnp.where(class_row == row, 1.0, 0.0).astype(BF)

    def features(s):
        index = jnp.full((32, 128), s, jnp.int32)
        return tuple(jnp.take_along_axis(ft[k], index, axis=1, mode="promise_in_bounds") for k in range(5))

    mine = [frequencies((first_tile(q) + h) * TILE) for h in range(2)]

    def weigh(s):
        feature = features(s)
        for half in range(2):
            wedge = wedge_of(feature, mine[half])
            where = (rows32(s), slice(half * 128, half * 128 + 128))
            wg[where] = wedge
            wlow[where] = wedge.astype(BF)
            wsq[where] = (wedge * wedge).astype(BF)

    over(0, NQ, weigh, unroll=2)

    contract = (((1,), (1,)), ((), ()))
    limits = (COEF, jnp.where(double, COEF, 0).astype(F32))
    valid = jnp.concatenate([jnp.where(mine[h][5] < limits[h], 1.0, 0.0) for h in range(2)], axis=1)
    valid = jnp.broadcast_to(valid, (8, WIDE)).astype(BF)
    total = lax.dot_general(valid, wlow[...], contract, preferred_element_type=F32)
    upper = total.astype(BF)
    rows = jnp.concatenate([jnp.ones((8, 1024), BF), upper, (total - upper.astype(F32)).astype(BF)], axis=0)
    found = lax.dot_general(rows, oh[...], contract, preferred_element_type=F32)
    s8[0:1] = found[0:1]
    s8[1:2] = found[8:9] + found[16:17]
    statz[0]()
    zs[pl.ds(z, 1)] = s8[...][None]

    db[...] = jnp.dot(oh[...], wsq[...], preferred_element_type=F32).astype(BF)
    denz[0]()
    dr[pl.ds(z, 1)] = db[rows32(z)][None]

    def weigh_half(h):
        def weight(s):
            wedge = wg[rows32(s), h * 128 : h * 128 + 128]
            block = xb[h, s].astype(F32)
            wx[h, rows32(s), 0:128] = (wedge * block[:, 0:128]).astype(BF)
            wx[h, rows32(s), 128:256] = (wedge * block[:, 128:256]).astype(BF)

        over(0, NQ, weight, unroll=4)

    def half_sums(h):
        nb[h] = jnp.dot(oh[...], wx[h], preferred_element_type=F32).astype(BF)
        numz[h][0]()
        nr[h, pl.ds(z, 1)] = nb[h, rows32(z)][None]

    def give_back(k, swap, mine, theirs):
        swap.wait_recv()

        def add_core(t):
            sm[k, t] = (mine[t, c] + theirs[t]).astype(BF)

        over(0, 16, add_core, unroll=4)
        backs[k][0]()
        b1[k, pl.ds(chip, 1)] = sm[k, pl.ds(chip, 1)]

    parts[0][1]()
    weigh_half(0)
    half_sums(0)

    refsz[1]()
    for plane in range(NZ):
        block = rr[plane].astype(F32)
        for k in range(NY):
            rf[k * 64 + plane * 8 : k * 64 + plane * 8 + 8, :] = block[8 * k : 8 * k + 8]
    for h in range(2):
        real = rf[:, h * 256 : h * 256 + 128]
        imag = rf[:, h * 256 + 128 : h * 256 + 256]
        rpow[:, h * 128 : h * 128 + 128] = (real * real + imag * imag).astype(BF)
    sbe[...] = lax.dot_general(wlow[...], rpow[...], contract, preferred_element_type=F32).reshape(16, 2, 32, CLASSES)
    swap_e.start()
    part_sum = lax.dot_general(wx[0], rf[:, 0:256].astype(BF), contract, preferred_element_type=F32)
    sbi[...] = part_sum.reshape(16, 2, 32, CLASSES)

    statz[1]()
    every = jnp.sum(zs[...], axis=0)
    here = every[1:2]
    tm[...] = jnp.where(z < 4, here[:, 0:128], here[:, 128:256])
    totals[0]()
    tmr[pl.ds(q, 1)] = tm[...][None]
    ids = lax.broadcasted_iota(jnp.int32, (CLASSES, CLASSES), 1)
    ids = ((ids >> 3) & 7) * 32 + (ids >> 6) * 8 + (ids & 7)
    order = jnp.where(lax.broadcasted_iota(jnp.int32, (CLASSES, CLASSES), 0) == ids, 1.0, 0.0).astype(BF)
    counts = jnp.broadcast_to(every[0:1], (8, CLASSES))
    upper = counts.astype(BF)
    rows = jnp.concatenate([upper, (counts - upper.astype(F32)).astype(BF)], axis=0)
    moved = jnp.dot(rows, order, preferred_element_type=F32)
    count_ref[...] = (moved[0:1] + moved[8:9]) * (CLASSES / PARTICLES)

    second_arrived()
    weigh_half(1)
    half_sums(1)
    part_sum = lax.dot_general(wx[1], rf[:, 256:512].astype(BF), contract, preferred_element_type=F32)
    sbi[...] += part_sum.reshape(16, 2, 32, CLASSES)
    swap_i.start()

    give_back(0, swap_e, sbe, pbe)
    give_back(1, swap_i, sbi, pbi)

    denz[1]()
    denom = jnp.sum(dr[...].astype(F32), axis=0)
    totals[1]()
    pad0[...] = jnp.broadcast_to(jnp.sum(tmr[...], axis=0), (128, 128)).T
    tail = pad0[pl.ds(pl.multiple_of((z % 4) * 32, 32), 32), 0:1]
    bottom = denom + TAU * (tail / COEF + 1.0)
    scale = 1.0 / bottom
    for h in range(2):
        numz[h][1]()
        top = jnp.sum(nr[h].astype(F32), axis=0)
        for part in range(2):
            lanes = slice(h * 128, h * 128 + 128)
            mb[:, part, lanes] = top[:, part * 128 : part * 128 + 128] * scale[:, lanes]
    means[0]()
    mr[pl.ds(q, 1)] = mb[pl.ds(q, 1)]

    backs[0][1]()
    energy = jnp.sum(b1[0].astype(F32), axis=0)
    backs[1][1]()
    inter = jnp.sum(b1[1].astype(F32), axis=0)
    score_ref[...] = inter / (
        math.sqrt(COEF) * jnp.sqrt((energy / COEF + EPS) * (power / COEF + EPS))
    )
    means[1]()
    for t in range(NQ):
        first = first_tile(t) * TILE
        size = min(TILE if t in SINGLE else WIDE, COEF - first)
        mean_ref[0, :, first : first + size] = mr[t, :, 0:size]
    for group in (mixed, parts[0], totals, means, refsz, denz, *numz, statz, *backs):
        group[2]()
    swap_e.wait_send()
    swap_i.wait_send()
    second_sent()


def leave(score_in, mean_in, count_in, score_ref, mean_ref, count_ref, send):
    copies = [
        pltpu.make_async_copy(score_in, score_ref, send.at[0]),
        pltpu.make_async_copy(mean_in, mean_ref, send.at[1]),
        pltpu.make_async_copy(count_in, count_ref, send.at[2]),
    ]
    for copy in copies:
        copy.start()
    for copy in copies:
        copy.wait()


def body(particles, references, assignment, orientation, tilt_range):
    def v(*shape, dtype=F32):
        return pltpu.VMEM(shape, dtype)

    sem = pltpu.SemaphoreType.DMA
    vm = pl.BlockSpec(memory_space=pltpu.VMEM)
    hbm = pl.BlockSpec(memory_space=pltpu.HBM)
    shapes = (
        jax.ShapeDtypeStruct((PART, CLASSES), F32),
        jax.ShapeDtypeStruct((1, 2, COEF), F32),
        jax.ShapeDtypeStruct((1, CLASSES), F32),
    )
    outs = pl.pallas_call(
        kernel,
        out_shape=shapes,
        in_specs=[hbm] * 5,
        out_specs=(vm,) * 3,
        scratch_shapes=[
            v(PART, 2, COEF, dtype=BF), v(1, 2, COEF, dtype=BF),
            v(1, PART, dtype=jnp.int32), v(1, PART, dtype=jnp.int32), v(2, PART, dtype=jnp.int32),
            v(NQ, 4, WIDE, dtype=BF), v(NQ, 4, WIDE, dtype=BF),
            v(2, NQ, PART, WIDE, dtype=BF), v(2, NQ, PART, WIDE, dtype=BF),
            v(1, 128), v(NQ, 1, 128),
            v(32, 2 * WIDE, dtype=BF), v(NZ, 32, 2 * WIDE, dtype=BF),
            v(2, CLASSES, WIDE, dtype=BF), v(2, NZ, 32, WIDE, dtype=BF),
            v(CLASSES, WIDE, dtype=BF), v(NZ, 32, WIDE, dtype=BF),
            v(2, CLASSES), v(NZ, 2, CLASSES),
            v(128, 128), v(5, 32, 128), v(32, 128),
            v(CLASSES, 1024, dtype=BF), v(1024, WIDE), v(1024, WIDE, dtype=BF), v(1024, WIDE, dtype=BF),
            v(2, 1024, WIDE, dtype=BF), v(CLASSES, 2 * WIDE), v(CLASSES, WIDE, dtype=BF),
            v(16, 2, 32, CLASSES), v(16, 2, 32, CLASSES), v(16, 32, CLASSES), v(16, 32, CLASSES),
            v(2, 16, 32, CLASSES, dtype=BF), v(2, 16, 32, CLASSES, dtype=BF), v(NQ, 2, WIDE), v(NQ, 2, WIDE),
        ] + [sem((2,)), sem((3,))] + [sem((2,))] * 6 + [sem] * 16,
        compiler_params=pltpu.CompilerParams(
            collective_id=0, has_side_effects=True
        ),
    )(particles, references, assignment.T, orientation[None], tilt_range)
    scores, means, counts = pl.pallas_call(
        leave, out_shape=shapes, in_specs=[vm] * 3, out_specs=(hbm,) * 3, scratch_shapes=[sem((3,))]
    )(*outs)
    return scores, means, counts[0]


def solution(mesh):
    split = Mesh(mesh.devices.reshape(NY, NZ, NX, NC), DOM)
    placed = (P(DOM, None, None), P(DOM, None, None), P(DOM, None), P(DOM), P(None, DOM))
    return jax.shard_map(
        body,
        mesh=split,
        in_specs=placed,
        out_specs=(P(DOM, None), P(DOM, None, None), P()),
        check_vma=False,
    )
```

```python
import math

import jax
import jax.numpy as jnp
from jax import lax
from jax.experimental import pallas as pl
from jax.experimental.pallas import tpu as pltpu
from jax.sharding import Mesh
from jax.sharding import PartitionSpec as P

GRID = 24
ORIENTS = 36
COEF = 7488
CLASSES = 256
PARTICLES = 8192
EPS = 1e-06
GAIN = 6.0
TAU = 0.5

NY, NZ, NX, NC = 4, 8, 4, 2
NQ = NY * NX * NC
PART = 32
WIDE = 256
TILE = 128
AROUND = (
    (2, 2), (1, 1), (3, 3), (1, 2), (3, 2), (1, 3), (3, 1), (2, 1), (2, 3),
    (0, 2), (2, 0), (0, 1), (1, 0), (0, 3), (3, 0),
)
PADDED = 59 * TILE
SINGLE = (1, 9, 17, 25, 31)
DOM = ("y", "z", "x", "c")
BF = jnp.bfloat16
F32 = jnp.float32


def first_tile(q):
    return 2 * q - (q + 6) // 8


def frequencies(base, lanes=128):
    index = (lax.broadcasted_iota(jnp.int32, (1, lanes), 1) + base).astype(F32)
    plane = jnp.floor((index + 0.5) * (1.0 / (GRID * GRID)))
    rest = index - plane * (GRID * GRID)
    col_x = jnp.floor((rest + 0.5) * (1.0 / GRID))
    col_z = rest - col_x * GRID
    half = GRID // 2
    freq_x = jnp.where(col_x < half, col_x, col_x - GRID)
    freq_z = jnp.where(col_z < half, col_z, col_z - GRID)
    square_z = freq_z * freq_z
    return freq_x, plane, square_z, square_z + 1.0, -2.0 * freq_z, index


def wedge_of(feature, freq):
    sine, cosine, cos_centre, sin_centre, cos_width = feature
    freq_x, freq_y, square_z, square_z1, minus_2z, _ = freq
    along = freq_y * cosine - freq_x * sine
    square = along * along
    turned = ((square - square_z) * cos_centre + (minus_2z * along) * sin_centre) / (square + square_z1)
    return 1.0 / (1.0 + jnp.exp(-GAIN * (turned - cos_width)))


def kernel(
    part_hbm, ref_hbm, cls_hbm, ori_hbm, tilt_hbm,
    score_ref, mean_ref, count_ref,
    raw, rawr, lab_c, lab_o, lab_t, cm, cb, xs, xb, tm, tmr,
    r1, rr, nb, nr, db, dr, s8, zs,
    pad0, ft, sel, oh, wg, wlow, wsq, wx, rf, rpow,
    sbi, sbe, pbi, pbe, sm, b1, mb, sv, cv,
    in_s, lab_s, out_s, x_s, x_r, nz_s, nz_r, b_s, b_r, c_s, c_r, t_s, t_r, m_s, m_r,
    rz_s, rz_r, dz_s, dz_r, sz_s, sz_r,
    pe_s, pe_r, pi_s, pi_r,
):
    y = lax.axis_index("y")
    z = lax.axis_index("z")
    x = lax.axis_index("x")
    c = lax.axis_index("c")
    q = y * 8 + x * 2 + c
    chip = y * 4 + x

    def to_chip(dy, dx, dc):
        ty, tx, tc = (y + dy) & 3, (x + dx) & 3, c ^ dc
        return (ty * 8 + tx * 2 + tc, ty * 4 + tx), {"y": ty, "z": z, "x": tx, "c": tc}

    def plane_peers():
        for dy, dx in AROUND:
            for dc in (0, 1):
                yield lambda dy=dy, dx=dx, dc=dc: to_chip(dy, dx, dc)
        yield lambda: to_chip(0, 0, 1)

    def chip_peers():
        for dy, dx in AROUND:
            yield lambda dy=dy, dx=dx: to_chip(dy, dx, 0)

    def z_peers():
        for d in (4, 3, 5, 2, 6, 1, 7):

            def peer(d=d):
                t = (z + d) & 7
                return (t, t), {"y": y, "z": t, "x": x, "c": c}

            yield peer

    other = {"y": y, "z": z, "x": x, "c": 1 - c}

    def over(first, last, step, unroll=1):
        def one(d, _):
            step(d)
            return 0

        lax.fori_loop(first, last, one, 0, unroll=unroll)

    def pair(t):
        return (t % 8 != 1) & (t != 31)

    def exchange(group, me, src, dst, blocks, send, recv, wants=None):
        peers, index = {"plane": (plane_peers, 0), "chip": (chip_peers, 1), "z": (z_peers, 0)}[group]

        def start():
            for peer in peers():
                ts, place = peer()
                t = ts[index]
                copy = pltpu.make_async_remote_copy(
                    src_ref=src(t), dst_ref=dst(me), send_sem=send, recv_sem=recv,
                    device_id=place, device_id_type=pl.DeviceIdType.MESH,
                )
                if wants is None:
                    copy.start()
                else:
                    pl.when(wants(t))(copy.start)

        def wait_recv():
            pltpu.make_async_copy(blocks, blocks, recv).wait()

        def wait_send():
            pltpu.make_async_copy(blocks, blocks, send).wait()

        return start, wait_recv, wait_send

    def rows32(t):
        return pl.ds(pl.multiple_of(t * 32, 32), 32)

    reads = [
        pltpu.make_async_copy(part_hbm, raw, in_s.at[0]),
        pltpu.make_async_copy(ref_hbm, rawr, in_s.at[1]),
        pltpu.make_async_copy(cls_hbm, lab_c, lab_s.at[0]),
        pltpu.make_async_copy(ori_hbm, lab_o, lab_s.at[1]),
        pltpu.make_async_copy(tilt_hbm, lab_t, lab_s.at[2]),
    ]
    for read in reads:
        read.start()

    barrier = pltpu.get_barrier_semaphore()

    for peers in (plane_peers, z_peers):
        for peer in peers():
            pl.semaphore_signal(barrier, inc=1, device_id=peer()[1], device_id_type=pl.DeviceIdType.MESH)

    few = pl.ds(0, NQ - 1)
    fewz = pl.ds(0, NZ - 1)
    mixed = exchange("plane", q, lambda t: cm.at[t], lambda s: cb.at[s], cb.at[few], c_s, c_r)

    def parts_of(h):
        return exchange(
            "plane", q, lambda t: xs.at[h, t], lambda s: xb.at[h, s], xb.at[h, few], x_s.at[h], x_r.at[h],
            pair if h else None,
        )

    parts = [parts_of(0), parts_of(1)]
    double = pair(q)

    def second_arrived():
        @pl.when(double)
        def _():
            parts[1][1]()

    def second_sent():
        for case, others in ((double, NQ - len(SINGLE) - 1), (jnp.logical_not(double), NQ - len(SINGLE))):

            @pl.when(case)
            def _():
                sent = xb.at[1, pl.ds(0, others)]
                pltpu.make_async_copy(sent, sent, x_s.at[1]).wait()

    totals = exchange("plane", q, lambda t: tm, lambda s: tmr.at[s], tmr.at[few], t_s, t_r)

    def means_of(tiles):
        lanes = pl.ds(pl.multiple_of(first_tile(q) * TILE, TILE), tiles * TILE)
        inside = slice(0, tiles * TILE)
        return (
            exchange("plane", q, lambda t: mb.at[t, :, inside], lambda s: mean_ref.at[0, :, lanes], mb.at[few, :, inside], m_s, m_r),
            pltpu.make_async_copy(mb.at[q, :, inside], mean_ref.at[0, :, lanes], out_s.at[2]),
            mean_ref.at[0, :, 0 : PADDED - tiles * TILE],
        )

    def means(step):
        for tiles, case in ((2, double), (1, jnp.logical_not(double))):

            @pl.when(case)
            def _():
                others, own, expected = means_of(tiles)
                if step == 0:
                    others[0]()
                    own.start()
                else:
                    pltpu.make_async_copy(expected, expected, m_r).wait()
                    others[2]()
                    own.wait()

    refsz = exchange("z", z, lambda t: r1, lambda s: rr.at[s], rr.at[fewz], rz_s, rz_r)
    denz = exchange("z", z, lambda t: db.at[rows32(t)], lambda s: dr.at[s], dr.at[fewz], dz_s, dz_r)

    def numz_of(h):
        return exchange(
            "z", z, lambda t: nb.at[h, rows32(t)], lambda s: nr.at[h, s], nr.at[h, fewz], nz_s.at[h], nz_r.at[h]
        )

    numz = [numz_of(0), numz_of(1)]
    statz = exchange("z", z, lambda t: s8, lambda s: zs.at[s], zs.at[fewz], sz_s, sz_r)

    def backs_of(k):
        return exchange(
            "chip", chip, lambda t: sm.at[k, t], lambda s: b1.at[k, s], b1.at[k, pl.ds(0, 15)], b_s.at[k], b_r.at[k]
        )

    backs = [backs_of(0), backs_of(1)]

    def to_other(src, dst, send, recv):
        return pltpu.make_async_remote_copy(
            src_ref=src.at[:, 1 - c], dst_ref=dst, send_sem=send, recv_sem=recv,
            device_id=other, device_id_type=pl.DeviceIdType.MESH,
        )

    swap_e = to_other(sbe, pbe, pe_s, pe_r)
    swap_i = to_other(sbi, pbi, pi_s, pi_r)
    put_scores = pltpu.make_async_copy(sv, score_ref, out_s.at[0])
    put_counts = pltpu.make_async_copy(cv, count_ref, out_s.at[1])

    for read in reads[2:]:
        read.wait()
    labels = jnp.concatenate([lab_c[...], lab_o[...], lab_t[0:1, :], lab_t[1:2, :]], axis=1).astype(F32)
    two_rows = jnp.concatenate([labels, jnp.zeros((1, 128), F32)], axis=0).astype(BF)
    cm[:, 2:4, 0:128] = jnp.broadcast_to(two_rows[None], (NQ, 2, 128))
    cm[:, 2:4, 128:256] = jnp.zeros((NQ, 2, 128), BF)
    reads[1].wait()
    for t in range(NQ):
        first = first_tile(t) * TILE
        size = min(TILE if t in SINGLE else WIDE, COEF - first)
        if size < WIDE:
            cm[t, 0:2, :] = jnp.zeros((2, WIDE), BF)
        cm[t, 0:2, 0:size] = rawr[0, :, first : first + size]

    reads[0].wait()

    for t in range(NQ):
        first = first_tile(t) * TILE
        size = min(TILE if t in SINGLE else WIDE, COEF - first)
        both = jnp.swapaxes(raw[:, :, first : first + size], 0, 1)
        for h in range(2):
            wide = min(TILE, size - h * TILE)
            if wide < TILE:
                xs[h, t] = jnp.zeros((PART, WIDE), BF)
            if wide > 0:
                for part in range(2):
                    xs[h, t, :, part * TILE : part * TILE + wide] = both[part, :, h * TILE : h * TILE + wide]
    pl.semaphore_wait(barrier, NQ - 1 + NZ - 1)

    mixed[0]()
    parts[0][0]()
    parts[1][0]()
    cb[pl.ds(q, 1)] = cm[pl.ds(q, 1)]

    @pl.when(jnp.logical_not(double))
    def _():
        xb[1] = jnp.zeros((NQ, PART, WIDE), BF)

    for h in range(2):
        xb[h, pl.ds(q, 1)] = xs[h, pl.ds(q, 1)]

    def features_of(turned):
        angle = turned[32:64] * (2.0 * math.pi / ORIENTS)
        low = -(40.0 + 1.5 * turned[64:96]) * (math.pi / 180.0)
        high = (40.0 + 1.5 * turned[96:128]) * (math.pi / 180.0)
        centre = low + high
        return jnp.sin(angle), jnp.cos(angle), jnp.cos(centre), jnp.sin(centre), jnp.cos(high - low)

    pad0[...] = jnp.broadcast_to(labels, (128, 128))
    own = features_of(pad0[...].T)

    def own_slice(s, power):
        for half in range(2):
            wedge = wedge_of(own, frequencies((first_tile(s) + half) * TILE))
            real = xs[half, s, :, 0:128].astype(F32)
            imag = xs[half, s, :, 128:256].astype(F32)
            power = power + wedge * (real * real + imag * imag)
        return power

    power = lax.fori_loop(0, NQ, own_slice, jnp.zeros((32, 128), F32), unroll=2)
    power = jnp.sum(power, axis=1, keepdims=True)

    mixed[1]()
    both = jnp.swapaxes(cb[:, 0:2, :], 0, 1)
    for h in range(2):
        for part in range(2):
            at = h * 256 + part * 128
            r1[:, at : at + 128] = both[part, :, h * 128 : h * 128 + 128]
    refsz[0]()
    rr[pl.ds(z, 1)] = r1[...][None]

    every = jnp.swapaxes(cb[:, 2:4, 0:128], 0, 1)[0].astype(F32)
    pad0[0:32, :] = every
    for k, feature in enumerate(features_of(pad0[...].T)):
        ft[k] = feature
    sub = lax.broadcasted_iota(jnp.int32, (32, 128), 0)
    cls = jnp.where(lax.broadcasted_iota(jnp.int32, (32, 128), 1) < 32, every, 0.0).astype(jnp.int32)
    in_plane = (((cls >> 3) & 7) * 32 + (cls >> 6) * 8 + (cls & 7)).astype(F32)
    chosen = in_plane
    for k in range(1, 4):
        chosen = jnp.where((sub & 3) == k, pltpu.roll(in_plane, 32 * k, 1), chosen)
    sel[...] = chosen
    class_row = lax.broadcasted_iota(jnp.int32, (CLASSES, 128), 0).astype(F32)
    for tile in range(8):
        row = jnp.sum(sel[4 * tile : 4 * tile + 4, :], axis=0, keepdims=True)
        oh[:, tile * 128 : tile * 128 + 128] = jnp.where(class_row == row, 1.0, 0.0).astype(BF)

    def features(s):
        index = jnp.full((32, 128), s, jnp.int32)
        return tuple(jnp.take_along_axis(ft[k], index, axis=1, mode="promise_in_bounds") for k in range(5))

    mine = [frequencies((first_tile(q) + h) * TILE) for h in range(2)]

    def weigh(s):
        feature = features(s)
        for half in range(2):
            wedge = wedge_of(feature, mine[half])
            where = (rows32(s), slice(half * 128, half * 128 + 128))
            wg[where] = wedge
            wlow[where] = wedge.astype(BF)
            wsq[where] = (wedge * wedge).astype(BF)

    over(0, NQ, weigh, unroll=2)

    contract = (((1,), (1,)), ((), ()))
    limits = (COEF, jnp.where(double, COEF, 0).astype(F32))
    valid = jnp.concatenate([jnp.where(mine[h][5] < limits[h], 1.0, 0.0) for h in range(2)], axis=1)
    valid = jnp.broadcast_to(valid, (8, WIDE)).astype(BF)
    total = lax.dot_general(valid, wlow[...], contract, preferred_element_type=F32)
    upper = total.astype(BF)
    rows = jnp.concatenate([jnp.ones((8, 1024), BF), upper, (total - upper.astype(F32)).astype(BF)], axis=0)
    found = lax.dot_general(rows, oh[...], contract, preferred_element_type=F32)
    s8[0:1] = found[0:1]
    s8[1:2] = found[8:9] + found[16:17]
    statz[0]()
    zs[pl.ds(z, 1)] = s8[...][None]

    db[...] = jnp.dot(oh[...], wsq[...], preferred_element_type=F32).astype(BF)
    denz[0]()
    dr[pl.ds(z, 1)] = db[rows32(z)][None]

    def weigh_half(h):
        def weight(s):
            wedge = wg[rows32(s), h * 128 : h * 128 + 128]
            block = xb[h, s].astype(F32)
            wx[h, rows32(s), 0:128] = (wedge * block[:, 0:128]).astype(BF)
            wx[h, rows32(s), 128:256] = (wedge * block[:, 128:256]).astype(BF)

        over(0, NQ, weight, unroll=4)

    def half_sums(h):
        nb[h] = jnp.dot(oh[...], wx[h], preferred_element_type=F32).astype(BF)
        numz[h][0]()
        nr[h, pl.ds(z, 1)] = nb[h, rows32(z)][None]

    def give_back(k, swap, mine, theirs):
        swap.wait_recv()

        def add_core(t):
            sm[k, t] = (mine[t, c] + theirs[t]).astype(BF)

        over(0, 16, add_core, unroll=4)
        backs[k][0]()
        b1[k, pl.ds(chip, 1)] = sm[k, pl.ds(chip, 1)]

    parts[0][1]()
    weigh_half(0)
    half_sums(0)

    refsz[1]()
    for plane in range(NZ):
        block = rr[plane].astype(F32)
        for k in range(NY):
            rf[k * 64 + plane * 8 : k * 64 + plane * 8 + 8, :] = block[8 * k : 8 * k + 8]
    for h in range(2):
        real = rf[:, h * 256 : h * 256 + 128]
        imag = rf[:, h * 256 + 128 : h * 256 + 256]
        rpow[:, h * 128 : h * 128 + 128] = (real * real + imag * imag).astype(BF)
    sbe[...] = lax.dot_general(wlow[...], rpow[...], contract, preferred_element_type=F32).reshape(16, 2, 32, CLASSES)
    swap_e.start()
    statz[1]()
    every = jnp.sum(zs[...], axis=0)
    here = every[1:2]
    tm[...] = jnp.where(z < 4, here[:, 0:128], here[:, 128:256])
    totals[0]()
    tmr[pl.ds(q, 1)] = tm[...][None]
    ids = lax.broadcasted_iota(jnp.int32, (CLASSES, CLASSES), 1)
    ids = ((ids >> 3) & 7) * 32 + (ids >> 6) * 8 + (ids & 7)
    order = jnp.where(lax.broadcasted_iota(jnp.int32, (CLASSES, CLASSES), 0) == ids, 1.0, 0.0).astype(BF)
    counts = jnp.broadcast_to(every[0:1], (8, CLASSES))
    upper = counts.astype(BF)
    rows = jnp.concatenate([upper, (counts - upper.astype(F32)).astype(BF)], axis=0)
    moved = jnp.dot(rows, order, preferred_element_type=F32)
    cv[...] = (moved[0:1] + moved[8:9]) * (CLASSES / PARTICLES)
    put_counts.start()

    second_arrived()
    weigh_half(1)
    half_sums(1)

    give_back(0, swap_e, sbe, pbe)

    part_sum = lax.dot_general(wx[0], rf[:, 0:256].astype(BF), contract, preferred_element_type=F32)
    part_sum = part_sum + lax.dot_general(wx[1], rf[:, 256:512].astype(BF), contract, preferred_element_type=F32)
    sbi[...] = part_sum.reshape(16, 2, 32, CLASSES)
    swap_i.start()
    give_back(1, swap_i, sbi, pbi)

    denz[1]()
    denom = jnp.sum(dr[...].astype(F32), axis=0)
    totals[1]()
    pad0[...] = jnp.broadcast_to(jnp.sum(tmr[...], axis=0), (128, 128)).T
    tail = pad0[pl.ds(pl.multiple_of((z % 4) * 32, 32), 32), 0:1]
    bottom = denom + TAU * (tail / COEF + 1.0)
    scale = 1.0 / bottom
    for h in range(2):
        numz[h][1]()
        top = jnp.sum(nr[h].astype(F32), axis=0)
        for part in range(2):
            lanes = slice(h * 128, h * 128 + 128)
            mb[:, part, lanes] = top[:, part * 128 : part * 128 + 128] * scale[:, lanes]
    means(0)

    backs[0][1]()
    energy = jnp.sum(b1[0].astype(F32), axis=0)
    backs[1][1]()
    inter = jnp.sum(b1[1].astype(F32), axis=0)
    sv[...] = inter / (
        math.sqrt(COEF) * jnp.sqrt((energy / COEF + EPS) * (power / COEF + EPS))
    )
    put_scores.start()
    means(1)
    for leaving in (put_counts, put_scores):
        leaving.wait()
    for group in (mixed, parts[0], totals, refsz, denz, *numz, statz, *backs):
        group[2]()
    swap_e.wait_send()
    swap_i.wait_send()
    second_sent()


def leave(score_in, mean_in, count_in, score_ref, mean_ref, count_ref):
    score_ref[...] = score_in[...]
    mean_ref[...] = mean_in[:, :, 0:COEF]
    count_ref[...] = count_in[...]


def body(particles, references, assignment, orientation, tilt_range):
    def v(*shape, dtype=F32):
        return pltpu.VMEM(shape, dtype)

    sem = pltpu.SemaphoreType.DMA
    vm = pl.BlockSpec(memory_space=pltpu.VMEM)
    hbm = pl.BlockSpec(memory_space=pltpu.HBM)
    def shapes(wide):
        return (
            jax.ShapeDtypeStruct((PART, CLASSES), F32),
            jax.ShapeDtypeStruct((1, 2, wide), F32),
            jax.ShapeDtypeStruct((1, CLASSES), F32),
        )

    outs = pl.pallas_call(
        kernel,
        out_shape=shapes(PADDED),
        in_specs=[hbm] * 5,
        out_specs=(hbm,) * 3,
        scratch_shapes=[
            v(PART, 2, COEF, dtype=BF), v(1, 2, COEF, dtype=BF),
            v(1, PART, dtype=jnp.int32), v(1, PART, dtype=jnp.int32), v(2, PART, dtype=jnp.int32),
            v(NQ, 4, WIDE, dtype=BF), v(NQ, 4, WIDE, dtype=BF),
            v(2, NQ, PART, WIDE, dtype=BF), v(2, NQ, PART, WIDE, dtype=BF),
            v(1, 128), v(NQ, 1, 128),
            v(32, 2 * WIDE, dtype=BF), v(NZ, 32, 2 * WIDE, dtype=BF),
            v(2, CLASSES, WIDE, dtype=BF), v(2, NZ, 32, WIDE, dtype=BF),
            v(CLASSES, WIDE, dtype=BF), v(NZ, 32, WIDE, dtype=BF),
            v(2, CLASSES), v(NZ, 2, CLASSES),
            v(128, 128), v(5, 32, 128), v(32, 128),
            v(CLASSES, 1024, dtype=BF), v(1024, WIDE), v(1024, WIDE, dtype=BF), v(1024, WIDE, dtype=BF),
            v(2, 1024, WIDE, dtype=BF), v(CLASSES, 2 * WIDE), v(CLASSES, WIDE, dtype=BF),
            v(16, 2, 32, CLASSES), v(16, 2, 32, CLASSES), v(16, 32, CLASSES), v(16, 32, CLASSES),
            v(2, 16, 32, CLASSES, dtype=BF), v(2, 16, 32, CLASSES, dtype=BF), v(NQ, 2, WIDE), v(PART, CLASSES), v(1, CLASSES),
        ] + [sem((2,)), sem((3,)), sem((3,))] + [sem((2,))] * 6 + [sem] * 16,
        compiler_params=pltpu.CompilerParams(
            collective_id=0, has_side_effects=True
        ),
    )(particles, references, assignment.T, orientation[None], tilt_range)
    scores, means, counts = pl.pallas_call(
        leave, out_shape=shapes(COEF), in_specs=[vm] * 3, out_specs=(vm,) * 3
    )(*outs)
    return scores, means, counts[0]


def solution(mesh):
    split = Mesh(mesh.devices.reshape(NY, NZ, NX, NC), DOM)
    placed = (P(DOM, None, None), P(DOM, None, None), P(DOM, None), P(DOM), P(None, DOM))
    return jax.shard_map(
        body,
        mesh=split,
        in_specs=placed,
        out_specs=(P(DOM, None), P(DOM, None, None), P()),
        check_vma=False,
    )
```

```python
import math

import jax
import jax.numpy as jnp
from jax import lax
from jax.experimental import pallas as pl
from jax.experimental.pallas import tpu as pltpu
from jax.sharding import Mesh
from jax.sharding import PartitionSpec as P

GRID = 24
ORIENTS = 36
COEF = 7488
CLASSES = 256
PARTICLES = 8192
EPS = 1e-06
GAIN = 6.0
TAU = 0.5

NY, NZ, NX, NC = 4, 8, 4, 2
NQ = NY * NX * NC
PART = 32
WIDE = 256
TILE = 128
OUTER = (
    (2, 2), (1, 1), (3, 3), (1, 2), (3, 2), (1, 3), (3, 1), (2, 1), (2, 3),
    (0, 2), (2, 0), (0, 1), (1, 0), (0, 3), (3, 0),
)
AROUND = (
    (0, 3), (0, 1), (3, 3), (1, 1), (3, 2), (1, 2), (2, 2), (1, 0), (3, 0), (2, 1), (2, 3), (2, 0), (0, 2), (1, 3), (3, 1),
)
PADDED = 59 * TILE
SINGLE = (1, 9, 17, 25, 31)
DOM = ("y", "z", "x", "c")
BF = jnp.bfloat16
F32 = jnp.float32


def first_tile(q):
    return 2 * q - (q + 6) // 8


def frequencies(base, lanes=128):
    index = (lax.broadcasted_iota(jnp.int32, (1, lanes), 1) + base).astype(F32)
    plane = jnp.floor((index + 0.5) * (1.0 / (GRID * GRID)))
    rest = index - plane * (GRID * GRID)
    col_x = jnp.floor((rest + 0.5) * (1.0 / GRID))
    col_z = rest - col_x * GRID
    half = GRID // 2
    freq_x = jnp.where(col_x < half, col_x, col_x - GRID)
    freq_z = jnp.where(col_z < half, col_z, col_z - GRID)
    square_z = freq_z * freq_z
    return freq_x, plane, square_z, square_z + 1.0, -2.0 * freq_z, index


def wedge_of(feature, freq):
    sine, cosine, cos_centre, sin_centre, cos_width = feature
    freq_x, freq_y, square_z, square_z1, minus_2z, _ = freq
    along = freq_y * cosine - freq_x * sine
    square = along * along
    turned = ((square - square_z) * cos_centre + (minus_2z * along) * sin_centre) / (square + square_z1)
    return 1.0 / (1.0 + jnp.exp(-GAIN * (turned - cos_width)))


def kernel(
    part_hbm, ref_hbm, cls_hbm, ori_hbm, tilt_hbm,
    score_ref, mean_ref, count_ref,
    raw, rawr, lab_c, lab_o, lab_t, cm, cb, xs, xb, tm, tmr,
    r1, rr, nb, nr, db, dr, s8, zs,
    pad0, ft, sel, oh, wg, wlow, wsq, wx, rf, rpow,
    sbi, sbe, pbi, pbe, sm, b1, mb, sv, cv,
    in_s, lab_s, out_s, x_s, x_r, nz_s, nz_r, b_s, b_r, c_s, c_r, t_s, t_r, m_s, m_r,
    rz_s, rz_r, dz_s, dz_r, sz_s, sz_r,
    pe_s, pe_r, pi_s, pi_r,
):
    y = lax.axis_index("y")
    z = lax.axis_index("z")
    x = lax.axis_index("x")
    c = lax.axis_index("c")
    q = y * 8 + x * 2 + c
    chip = y * 4 + x

    def to_chip(dy, dx, dc):
        ty, tx, tc = (y + dy) & 3, (x + dx) & 3, c ^ dc
        return (ty * 8 + tx * 2 + tc, ty * 4 + tx), {"y": ty, "z": z, "x": tx, "c": tc}

    def plane_peers(around=AROUND):
        for dy, dx in around:
            for dc in (0, 1):
                yield lambda dy=dy, dx=dx, dc=dc: to_chip(dy, dx, dc)
        yield lambda: to_chip(0, 0, 1)

    def chip_peers(around=AROUND):
        for dy, dx in around:
            yield lambda dy=dy, dx=dx: to_chip(dy, dx, 0)

    def z_peers():
        for d in (4, 3, 5, 2, 6, 1, 7):

            def peer(d=d):
                t = (z + d) & 7
                return (t, t), {"y": y, "z": t, "x": x, "c": c}

            yield peer

    other = {"y": y, "z": z, "x": x, "c": 1 - c}

    def over(first, last, step, unroll=1):
        def one(d, _):
            step(d)
            return 0

        lax.fori_loop(first, last, one, 0, unroll=unroll)

    def pair(t):
        return (t % 8 != 1) & (t != 31)

    def exchange(group, me, src, dst, blocks, send, recv, wants=None, around=AROUND):
        peers, index = {"plane": (plane_peers, 0), "chip": (chip_peers, 1), "z": (z_peers, 0)}[group]

        def start():
            for peer in peers(*(() if group == "z" else (around,))):
                ts, place = peer()
                t = ts[index]
                copy = pltpu.make_async_remote_copy(
                    src_ref=src(t), dst_ref=dst(me), send_sem=send, recv_sem=recv,
                    device_id=place, device_id_type=pl.DeviceIdType.MESH,
                )
                if wants is None:
                    copy.start()
                else:
                    pl.when(wants(t))(copy.start)

        def wait_recv():
            pltpu.make_async_copy(blocks, blocks, recv).wait()

        def wait_send():
            pltpu.make_async_copy(blocks, blocks, send).wait()

        return start, wait_recv, wait_send

    def rows32(t):
        return pl.ds(pl.multiple_of(t * 32, 32), 32)

    reads = [
        pltpu.make_async_copy(part_hbm, raw, in_s.at[0]),
        pltpu.make_async_copy(ref_hbm, rawr, in_s.at[1]),
        pltpu.make_async_copy(cls_hbm, lab_c, lab_s.at[0]),
        pltpu.make_async_copy(ori_hbm, lab_o, lab_s.at[1]),
        pltpu.make_async_copy(tilt_hbm, lab_t, lab_s.at[2]),
    ]
    for read in reads:
        read.start()

    barrier = pltpu.get_barrier_semaphore()

    for peers in (plane_peers, z_peers):
        for peer in peers():
            pl.semaphore_signal(barrier, inc=1, device_id=peer()[1], device_id_type=pl.DeviceIdType.MESH)

    few = pl.ds(0, NQ - 1)
    fewz = pl.ds(0, NZ - 1)
    mixed = exchange("plane", q, lambda t: cm.at[t], lambda s: cb.at[s], cb.at[few], c_s, c_r)

    def parts_of(h):
        return exchange(
            "plane", q, lambda t: xs.at[h, t], lambda s: xb.at[h, s], xb.at[h, few], x_s.at[h], x_r.at[h],
            pair if h else None,
        )

    parts = [parts_of(0), parts_of(1)]
    double = pair(q)

    def second_arrived():
        @pl.when(double)
        def _():
            parts[1][1]()

    def second_sent():
        for case, others in ((double, NQ - len(SINGLE) - 1), (jnp.logical_not(double), NQ - len(SINGLE))):

            @pl.when(case)
            def _():
                sent = xb.at[1, pl.ds(0, others)]
                pltpu.make_async_copy(sent, sent, x_s.at[1]).wait()

    totals = exchange("plane", q, lambda t: tm, lambda s: tmr.at[s], tmr.at[few], t_s, t_r)

    def means_of(tiles):
        lanes = pl.ds(pl.multiple_of(first_tile(q) * TILE, TILE), tiles * TILE)
        inside = slice(0, tiles * TILE)
        return (
            exchange("plane", q, lambda t: mb.at[t, :, inside], lambda s: mean_ref.at[0, :, lanes], mb.at[few, :, inside], m_s, m_r, None, OUTER),
            pltpu.make_async_copy(mb.at[q, :, inside], mean_ref.at[0, :, lanes], out_s.at[2]),
            mean_ref.at[0, :, 0 : PADDED - tiles * TILE],
        )

    def means(step):
        for tiles, case in ((2, double), (1, jnp.logical_not(double))):

            @pl.when(case)
            def _():
                others, own, expected = means_of(tiles)
                if step == 0:
                    others[0]()
                    own.start()
                else:
                    pltpu.make_async_copy(expected, expected, m_r).wait()
                    others[2]()
                    own.wait()

    refsz = exchange("z", z, lambda t: r1, lambda s: rr.at[s], rr.at[fewz], rz_s, rz_r)
    denz = exchange("z", z, lambda t: db.at[rows32(t)], lambda s: dr.at[s], dr.at[fewz], dz_s, dz_r)

    def numz_of(h):
        return exchange(
            "z", z, lambda t: nb.at[h, rows32(t)], lambda s: nr.at[h, s], nr.at[h, fewz], nz_s.at[h], nz_r.at[h]
        )

    numz = [numz_of(0), numz_of(1)]
    statz = exchange("z", z, lambda t: s8, lambda s: zs.at[s], zs.at[fewz], sz_s, sz_r)

    def backs_of(k):
        return exchange(
            "chip", chip, lambda t: sm.at[k, t], lambda s: b1.at[k, s], b1.at[k, pl.ds(0, 15)], b_s.at[k], b_r.at[k], None, OUTER
        )

    backs = [backs_of(0), backs_of(1)]

    def to_other(src, dst, send, recv):
        return pltpu.make_async_remote_copy(
            src_ref=src.at[:, 1 - c], dst_ref=dst, send_sem=send, recv_sem=recv,
            device_id=other, device_id_type=pl.DeviceIdType.MESH,
        )

    swap_e = to_other(sbe, pbe, pe_s, pe_r)
    swap_i = to_other(sbi, pbi, pi_s, pi_r)
    put_scores = pltpu.make_async_copy(sv, score_ref, out_s.at[0])
    put_counts = pltpu.make_async_copy(cv, count_ref, out_s.at[1])

    for read in reads[2:]:
        read.wait()
    labels = jnp.concatenate([lab_c[...], lab_o[...], lab_t[0:1, :], lab_t[1:2, :]], axis=1).astype(F32)
    two_rows = jnp.concatenate([labels, jnp.zeros((1, 128), F32)], axis=0).astype(BF)
    cm[:, 2:4, 0:128] = jnp.broadcast_to(two_rows[None], (NQ, 2, 128))
    cm[:, 2:4, 128:256] = jnp.zeros((NQ, 2, 128), BF)
    reads[1].wait()
    for t in range(NQ):
        first = first_tile(t) * TILE
        size = min(TILE if t in SINGLE else WIDE, COEF - first)
        if size < WIDE:
            cm[t, 0:2, :] = jnp.zeros((2, WIDE), BF)
        cm[t, 0:2, 0:size] = rawr[0, :, first : first + size]

    reads[0].wait()

    for t in range(NQ):
        first = first_tile(t) * TILE
        size = min(TILE if t in SINGLE else WIDE, COEF - first)
        both = jnp.swapaxes(raw[:, :, first : first + size], 0, 1)
        for h in range(2):
            wide = min(TILE, size - h * TILE)
            if wide < TILE:
                xs[h, t] = jnp.zeros((PART, WIDE), BF)
            if wide > 0:
                for part in range(2):
                    xs[h, t, :, part * TILE : part * TILE + wide] = both[part, :, h * TILE : h * TILE + wide]
    pl.semaphore_wait(barrier, NQ - 1 + NZ - 1)

    mixed[0]()
    parts[0][0]()
    parts[1][0]()
    cb[pl.ds(q, 1)] = cm[pl.ds(q, 1)]

    @pl.when(jnp.logical_not(double))
    def _():
        xb[1] = jnp.zeros((NQ, PART, WIDE), BF)

    for h in range(2):
        xb[h, pl.ds(q, 1)] = xs[h, pl.ds(q, 1)]

    def features_of(turned):
        angle = turned[32:64] * (2.0 * math.pi / ORIENTS)
        low = -(40.0 + 1.5 * turned[64:96]) * (math.pi / 180.0)
        high = (40.0 + 1.5 * turned[96:128]) * (math.pi / 180.0)
        centre = low + high
        return jnp.sin(angle), jnp.cos(angle), jnp.cos(centre), jnp.sin(centre), jnp.cos(high - low)

    pad0[...] = jnp.broadcast_to(labels, (128, 128))
    own = features_of(pad0[...].T)

    def own_slice(s, power):
        for half in range(2):
            wedge = wedge_of(own, frequencies((first_tile(s) + half) * TILE))
            real = xs[half, s, :, 0:128].astype(F32)
            imag = xs[half, s, :, 128:256].astype(F32)
            power = power + wedge * (real * real + imag * imag)
        return power

    power = lax.fori_loop(0, NQ, own_slice, jnp.zeros((32, 128), F32), unroll=2)
    power = jnp.sum(power, axis=1, keepdims=True)

    mixed[1]()
    both = jnp.swapaxes(cb[:, 0:2, :], 0, 1)
    for h in range(2):
        for part in range(2):
            at = h * 256 + part * 128
            r1[:, at : at + 128] = both[part, :, h * 128 : h * 128 + 128]
    refsz[0]()
    rr[pl.ds(z, 1)] = r1[...][None]

    every = jnp.swapaxes(cb[:, 2:4, 0:128], 0, 1)[0].astype(F32)
    pad0[0:32, :] = every
    for k, feature in enumerate(features_of(pad0[...].T)):
        ft[k] = feature
    sub = lax.broadcasted_iota(jnp.int32, (32, 128), 0)
    cls = jnp.where(lax.broadcasted_iota(jnp.int32, (32, 128), 1) < 32, every, 0.0).astype(jnp.int32)
    in_plane = (((cls >> 3) & 7) * 32 + (cls >> 6) * 8 + (cls & 7)).astype(F32)
    chosen = in_plane
    for k in range(1, 4):
        chosen = jnp.where((sub & 3) == k, pltpu.roll(in_plane, 32 * k, 1), chosen)
    sel[...] = chosen
    class_row = lax.broadcasted_iota(jnp.int32, (CLASSES, 128), 0).astype(F32)
    for tile in range(8):
        row = jnp.sum(sel[4 * tile : 4 * tile + 4, :], axis=0, keepdims=True)
        oh[:, tile * 128 : tile * 128 + 128] = jnp.where(class_row == row, 1.0, 0.0).astype(BF)

    def features(s):
        index = jnp.full((32, 128), s, jnp.int32)
        return tuple(jnp.take_along_axis(ft[k], index, axis=1, mode="promise_in_bounds") for k in range(5))

    mine = [frequencies((first_tile(q) + h) * TILE) for h in range(2)]

    def weigh(s):
        feature = features(s)
        for half in range(2):
            wedge = wedge_of(feature, mine[half])
            where = (rows32(s), slice(half * 128, half * 128 + 128))
            wg[where] = wedge
            wlow[where] = wedge.astype(BF)
            wsq[where] = (wedge * wedge).astype(BF)

    over(0, NQ, weigh, unroll=2)

    contract = (((1,), (1,)), ((), ()))
    limits = (COEF, jnp.where(double, COEF, 0).astype(F32))
    valid = jnp.concatenate([jnp.where(mine[h][5] < limits[h], 1.0, 0.0) for h in range(2)], axis=1)
    valid = jnp.broadcast_to(valid, (8, WIDE)).astype(BF)
    total = lax.dot_general(valid, wlow[...], contract, preferred_element_type=F32)
    upper = total.astype(BF)
    rows = jnp.concatenate([jnp.ones((8, 1024), BF), upper, (total - upper.astype(F32)).astype(BF)], axis=0)
    found = lax.dot_general(rows, oh[...], contract, preferred_element_type=F32)
    s8[0:1] = found[0:1]
    s8[1:2] = found[8:9] + found[16:17]
    statz[0]()
    zs[pl.ds(z, 1)] = s8[...][None]

    db[...] = jnp.dot(oh[...], wsq[...], preferred_element_type=F32).astype(BF)
    denz[0]()
    dr[pl.ds(z, 1)] = db[rows32(z)][None]

    def weigh_half(h):
        def weight(s):
            wedge = wg[rows32(s), h * 128 : h * 128 + 128]
            block = xb[h, s].astype(F32)
            wx[h, rows32(s), 0:128] = (wedge * block[:, 0:128]).astype(BF)
            wx[h, rows32(s), 128:256] = (wedge * block[:, 128:256]).astype(BF)

        over(0, NQ, weight, unroll=4)

    def half_sums(h):
        nb[h] = jnp.dot(oh[...], wx[h], preferred_element_type=F32).astype(BF)
        numz[h][0]()
        nr[h, pl.ds(z, 1)] = nb[h, rows32(z)][None]

    def give_back(k, swap, mine, theirs):
        swap.wait_recv()

        def add_core(t):
            sm[k, t] = (mine[t, c] + theirs[t]).astype(BF)

        over(0, 16, add_core, unroll=4)
        backs[k][0]()
        b1[k, pl.ds(chip, 1)] = sm[k, pl.ds(chip, 1)]

    parts[0][1]()
    weigh_half(0)
    half_sums(0)

    refsz[1]()
    for plane in range(NZ):
        block = rr[plane].astype(F32)
        for k in range(NY):
            rf[k * 64 + plane * 8 : k * 64 + plane * 8 + 8, :] = block[8 * k : 8 * k + 8]
    for h in range(2):
        real = rf[:, h * 256 : h * 256 + 128]
        imag = rf[:, h * 256 + 128 : h * 256 + 256]
        rpow[:, h * 128 : h * 128 + 128] = (real * real + imag * imag).astype(BF)
    sbe[...] = lax.dot_general(wlow[...], rpow[...], contract, preferred_element_type=F32).reshape(16, 2, 32, CLASSES)
    swap_e.start()
    statz[1]()
    every = jnp.sum(zs[...], axis=0)
    here = every[1:2]
    tm[...] = jnp.where(z < 4, here[:, 0:128], here[:, 128:256])
    totals[0]()
    tmr[pl.ds(q, 1)] = tm[...][None]
    ids = lax.broadcasted_iota(jnp.int32, (CLASSES, CLASSES), 1)
    ids = ((ids >> 3) & 7) * 32 + (ids >> 6) * 8 + (ids & 7)
    order = jnp.where(lax.broadcasted_iota(jnp.int32, (CLASSES, CLASSES), 0) == ids, 1.0, 0.0).astype(BF)
    counts = jnp.broadcast_to(every[0:1], (8, CLASSES))
    upper = counts.astype(BF)
    rows = jnp.concatenate([upper, (counts - upper.astype(F32)).astype(BF)], axis=0)
    moved = jnp.dot(rows, order, preferred_element_type=F32)
    cv[...] = (moved[0:1] + moved[8:9]) * (CLASSES / PARTICLES)
    put_counts.start()

    give_back(0, swap_e, sbe, pbe)
    second_arrived()
    weigh_half(1)
    half_sums(1)


    part_sum = lax.dot_general(wx[0], rf[:, 0:256].astype(BF), contract, preferred_element_type=F32)
    part_sum = part_sum + lax.dot_general(wx[1], rf[:, 256:512].astype(BF), contract, preferred_element_type=F32)
    sbi[...] = part_sum.reshape(16, 2, 32, CLASSES)
    swap_i.start()
    give_back(1, swap_i, sbi, pbi)

    denz[1]()
    denom = jnp.sum(dr[...].astype(F32), axis=0)
    totals[1]()
    pad0[...] = jnp.broadcast_to(jnp.sum(tmr[...], axis=0), (128, 128)).T
    tail = pad0[pl.ds(pl.multiple_of((z % 4) * 32, 32), 32), 0:1]
    bottom = denom + TAU * (tail / COEF + 1.0)
    scale = 1.0 / bottom
    for h in range(2):
        numz[h][1]()
        top = jnp.sum(nr[h].astype(F32), axis=0)
        for part in range(2):
            lanes = slice(h * 128, h * 128 + 128)
            mb[:, part, lanes] = top[:, part * 128 : part * 128 + 128] * scale[:, lanes]
    means(0)

    backs[0][1]()
    energy = jnp.sum(b1[0].astype(F32), axis=0)
    backs[1][1]()
    inter = jnp.sum(b1[1].astype(F32), axis=0)
    sv[...] = inter / (
        math.sqrt(COEF) * jnp.sqrt((energy / COEF + EPS) * (power / COEF + EPS))
    )
    put_scores.start()
    means(1)
    for leaving in (put_counts, put_scores):
        leaving.wait()
    for group in (mixed, parts[0], totals, refsz, denz, *numz, statz, *backs):
        group[2]()
    swap_e.wait_send()
    swap_i.wait_send()
    second_sent()


def leave(score_in, mean_in, count_in, score_ref, mean_ref, count_ref):
    score_ref[...] = score_in[...]
    mean_ref[...] = mean_in[:, :, 0:COEF]
    count_ref[...] = count_in[...]


def body(particles, references, assignment, orientation, tilt_range):
    def v(*shape, dtype=F32):
        return pltpu.VMEM(shape, dtype)

    sem = pltpu.SemaphoreType.DMA
    vm = pl.BlockSpec(memory_space=pltpu.VMEM)
    hbm = pl.BlockSpec(memory_space=pltpu.HBM)
    def shapes(wide):
        return (
            jax.ShapeDtypeStruct((PART, CLASSES), F32),
            jax.ShapeDtypeStruct((1, 2, wide), F32),
            jax.ShapeDtypeStruct((1, CLASSES), F32),
        )

    outs = pl.pallas_call(
        kernel,
        out_shape=shapes(PADDED),
        in_specs=[hbm] * 5,
        out_specs=(hbm,) * 3,
        scratch_shapes=[
            v(PART, 2, COEF, dtype=BF), v(1, 2, COEF, dtype=BF),
            v(1, PART, dtype=jnp.int32), v(1, PART, dtype=jnp.int32), v(2, PART, dtype=jnp.int32),
            v(NQ, 4, WIDE, dtype=BF), v(NQ, 4, WIDE, dtype=BF),
            v(2, NQ, PART, WIDE, dtype=BF), v(2, NQ, PART, WIDE, dtype=BF),
            v(1, 128), v(NQ, 1, 128),
            v(32, 2 * WIDE, dtype=BF), v(NZ, 32, 2 * WIDE, dtype=BF),
            v(2, CLASSES, WIDE, dtype=BF), v(2, NZ, 32, WIDE, dtype=BF),
            v(CLASSES, WIDE, dtype=BF), v(NZ, 32, WIDE, dtype=BF),
            v(2, CLASSES), v(NZ, 2, CLASSES),
            v(128, 128), v(5, 32, 128), v(32, 128),
            v(CLASSES, 1024, dtype=BF), v(1024, WIDE), v(1024, WIDE, dtype=BF), v(1024, WIDE, dtype=BF),
            v(2, 1024, WIDE, dtype=BF), v(CLASSES, 2 * WIDE), v(CLASSES, WIDE, dtype=BF),
            v(16, 2, 32, CLASSES), v(16, 2, 32, CLASSES), v(16, 32, CLASSES), v(16, 32, CLASSES),
            v(2, 16, 32, CLASSES, dtype=BF), v(2, 16, 32, CLASSES, dtype=BF), v(NQ, 2, WIDE), v(PART, CLASSES), v(1, CLASSES),
        ] + [sem((2,)), sem((3,)), sem((3,))] + [sem((2,))] * 6 + [sem] * 16,
        compiler_params=pltpu.CompilerParams(
            collective_id=0, has_side_effects=True
        ),
    )(particles, references, assignment.T, orientation[None], tilt_range)
    scores, means, counts = pl.pallas_call(
        leave, out_shape=shapes(COEF), in_specs=[vm] * 3, out_specs=(vm,) * 3
    )(*outs)
    return scores, means, counts[0]


def solution(mesh):
    split = Mesh(mesh.devices.reshape(NY, NZ, NX, NC), DOM)
    placed = (P(DOM, None, None), P(DOM, None, None), P(DOM, None), P(DOM), P(None, DOM))
    return jax.shard_map(
        body,
        mesh=split,
        in_specs=placed,
        out_specs=(P(DOM, None), P(DOM, None, None), P()),
        check_vma=False,
    )
```

```python
import math

import jax
import jax.numpy as jnp
from jax import lax
from jax.experimental import pallas as pl
from jax.experimental.pallas import tpu as pltpu
from jax.sharding import Mesh
from jax.sharding import PartitionSpec as P

GRID = 24
ORIENTS = 36
COEF = 7488
CLASSES = 256
PARTICLES = 8192
EPS = 1e-06
GAIN = 6.0
TAU = 0.5

NY, NZ, NX, NC = 4, 8, 4, 2
NQ = NY * NX * NC
PART = 32
WIDE = 256
TILE = 128
OUTER = (
    (2, 2), (1, 1), (3, 3), (1, 2), (3, 2), (1, 3), (3, 1), (2, 1), (2, 3),
    (0, 2), (2, 0), (0, 1), (1, 0), (0, 3), (3, 0),
)
AROUND = (
    (0, 3), (0, 1), (3, 3), (1, 1), (3, 2), (1, 2), (2, 2), (1, 0), (3, 0), (2, 1), (2, 3), (2, 0), (0, 2), (1, 3), (3, 1),
)
PADDED = 59 * TILE
SINGLE = (1, 9, 17, 25, 31)
DOM = ("y", "z", "x", "c")
BF = jnp.bfloat16
F32 = jnp.float32


def first_tile(q):
    return 2 * q - (q + 6) // 8


def frequencies(base, lanes=128):
    index = (lax.broadcasted_iota(jnp.int32, (1, lanes), 1) + base).astype(F32)
    plane = jnp.floor((index + 0.5) * (1.0 / (GRID * GRID)))
    rest = index - plane * (GRID * GRID)
    col_x = jnp.floor((rest + 0.5) * (1.0 / GRID))
    col_z = rest - col_x * GRID
    half = GRID // 2
    freq_x = jnp.where(col_x < half, col_x, col_x - GRID)
    freq_z = jnp.where(col_z < half, col_z, col_z - GRID)
    square_z = freq_z * freq_z
    return freq_x, plane, square_z, square_z + 1.0, -2.0 * freq_z, index


def wedge_of(feature, freq):
    sine, cosine, cos_centre, sin_centre, cos_width = feature
    freq_x, freq_y, square_z, square_z1, minus_2z, _ = freq
    along = freq_y * cosine - freq_x * sine
    square = along * along
    turned = ((square - square_z) * cos_centre + (minus_2z * along) * sin_centre) / (square + square_z1)
    return 1.0 / (1.0 + jnp.exp(-GAIN * (turned - cos_width)))


def kernel(
    part_hbm, ref_hbm, cls_hbm, ori_hbm, tilt_hbm,
    score_ref, mean_ref, count_ref,
    raw, rawr, lab_c, lab_o, lab_t, cm, cb, xs, xb, tm, tmr,
    r1, rr, nb, nr, db, dr, s8, zs,
    pad0, ft, sel, oh, wg, wlow, wsq, wx, rf, rpow,
    sbi, sbe, pbi, pbe, sm, b1, mb, sv, cv,
    in_s, lab_s, out_s, x_s, x_r, nz_s, nz_r, b_s, b_r, c_s, c_r, t_s, t_r, m_s, m_r,
    rz_s, rz_r, dz_s, dz_r, sz_s, sz_r,
    pe_s, pe_r, pi_s, pi_r,
):
    y = lax.axis_index("y")
    z = lax.axis_index("z")
    x = lax.axis_index("x")
    c = lax.axis_index("c")
    q = y * 8 + x * 2 + c
    chip = y * 4 + x

    def to_chip(dy, dx, dc):
        ty, tx, tc = (y + dy) & 3, (x + dx) & 3, c ^ dc
        return (ty * 8 + tx * 2 + tc, ty * 4 + tx), {"y": ty, "z": z, "x": tx, "c": tc}

    def plane_peers(around=AROUND):
        for dy, dx in around:
            for dc in (0, 1):
                yield lambda dy=dy, dx=dx, dc=dc: to_chip(dy, dx, dc)
        yield lambda: to_chip(0, 0, 1)

    def chip_peers(around=AROUND):
        for dy, dx in around:
            yield lambda dy=dy, dx=dx: to_chip(dy, dx, 0)

    def z_peers():
        for d in (4, 3, 5, 2, 6, 1, 7):

            def peer(d=d):
                t = (z + d) & 7
                return (t, t), {"y": y, "z": t, "x": x, "c": c}

            yield peer

    other = {"y": y, "z": z, "x": x, "c": 1 - c}

    def over(first, last, step, unroll=1):
        def one(d, _):
            step(d)
            return 0

        lax.fori_loop(first, last, one, 0, unroll=unroll)

    def pair(t):
        return (t % 8 != 1) & (t != 31)

    def exchange(group, me, src, dst, blocks, send, recv, wants=None, around=AROUND):
        peers, index = {"plane": (plane_peers, 0), "chip": (chip_peers, 1), "z": (z_peers, 0)}[group]

        def start():
            for peer in peers(*(() if group == "z" else (around,))):
                ts, place = peer()
                t = ts[index]
                copy = pltpu.make_async_remote_copy(
                    src_ref=src(t), dst_ref=dst(me), send_sem=send, recv_sem=recv,
                    device_id=place, device_id_type=pl.DeviceIdType.MESH,
                )
                if wants is None:
                    copy.start()
                else:
                    pl.when(wants(t))(copy.start)

        def wait_recv():
            pltpu.make_async_copy(blocks, blocks, recv).wait()

        def wait_send():
            pltpu.make_async_copy(blocks, blocks, send).wait()

        return start, wait_recv, wait_send

    def rows32(t):
        return pl.ds(pl.multiple_of(t * 32, 32), 32)

    reads = [
        pltpu.make_async_copy(part_hbm, raw, in_s.at[0]),
        pltpu.make_async_copy(ref_hbm, rawr, in_s.at[1]),
        pltpu.make_async_copy(cls_hbm, lab_c, lab_s.at[0]),
        pltpu.make_async_copy(ori_hbm, lab_o, lab_s.at[1]),
        pltpu.make_async_copy(tilt_hbm, lab_t, lab_s.at[2]),
    ]
    for read in reads:
        read.start()

    barrier = pltpu.get_barrier_semaphore()

    for peers in (plane_peers, z_peers):
        for peer in peers():
            pl.semaphore_signal(barrier, inc=1, device_id=peer()[1], device_id_type=pl.DeviceIdType.MESH)

    few = pl.ds(0, NQ - 1)
    fewz = pl.ds(0, NZ - 1)
    mixed = exchange("plane", q, lambda t: cm.at[t], lambda s: cb.at[s], cb.at[few], c_s, c_r)

    def parts_of(h):
        return exchange(
            "plane", q, lambda t: xs.at[h, t], lambda s: xb.at[h, s], xb.at[h, few], x_s.at[h], x_r.at[h],
            pair if h else None,
        )

    parts = [parts_of(0), parts_of(1)]
    double = pair(q)

    def second_arrived():
        @pl.when(double)
        def _():
            parts[1][1]()

    def second_sent():
        for case, others in ((double, NQ - len(SINGLE) - 1), (jnp.logical_not(double), NQ - len(SINGLE))):

            @pl.when(case)
            def _():
                sent = xb.at[1, pl.ds(0, others)]
                pltpu.make_async_copy(sent, sent, x_s.at[1]).wait()

    totals = exchange("plane", q, lambda t: tm, lambda s: tmr.at[s], tmr.at[few], t_s, t_r)

    def means_of(tiles):
        lanes = pl.ds(pl.multiple_of(first_tile(q) * TILE, TILE), tiles * TILE)
        inside = slice(0, tiles * TILE)
        return (
            exchange("plane", q, lambda t: mb.at[t, :, inside], lambda s: mean_ref.at[0, :, lanes], mb.at[few, :, inside], m_s, m_r, None, OUTER),
            pltpu.make_async_copy(mb.at[q, :, inside], mean_ref.at[0, :, lanes], out_s.at[2]),
            mean_ref.at[0, :, 0 : PADDED - tiles * TILE],
        )

    def means(step):
        for tiles, case in ((2, double), (1, jnp.logical_not(double))):

            @pl.when(case)
            def _():
                others, own, expected = means_of(tiles)
                if step == 0:
                    others[0]()
                    own.start()
                else:
                    pltpu.make_async_copy(expected, expected, m_r).wait()
                    others[2]()
                    own.wait()

    refsz = exchange("z", z, lambda t: r1, lambda s: rr.at[s], rr.at[fewz], rz_s, rz_r)
    denz = exchange("z", z, lambda t: db.at[rows32(t)], lambda s: dr.at[s], dr.at[fewz], dz_s, dz_r)

    def numz_of(h):
        return exchange(
            "z", z, lambda t: nb.at[h, rows32(t)], lambda s: nr.at[h, s], nr.at[h, fewz], nz_s.at[h], nz_r.at[h]
        )

    numz = [numz_of(0), numz_of(1)]
    statz = exchange("z", z, lambda t: s8, lambda s: zs.at[s], zs.at[fewz], sz_s, sz_r)

    def backs_of(k):
        return exchange(
            "chip", chip, lambda t: sm.at[k, t], lambda s: b1.at[k, s], b1.at[k, pl.ds(0, 15)], b_s.at[k], b_r.at[k], None, OUTER
        )

    backs = [backs_of(0), backs_of(1)]

    def to_other(src, dst, send, recv):
        return pltpu.make_async_remote_copy(
            src_ref=src.at[:, 1 - c], dst_ref=dst, send_sem=send, recv_sem=recv,
            device_id=other, device_id_type=pl.DeviceIdType.MESH,
        )

    swap_e = to_other(sbe, pbe, pe_s, pe_r)
    swap_i = to_other(sbi, pbi, pi_s, pi_r)
    put_scores = pltpu.make_async_copy(sv, score_ref, out_s.at[0])
    put_counts = pltpu.make_async_copy(cv, count_ref, out_s.at[1])

    for read in reads[2:]:
        read.wait()
    labels = jnp.concatenate([lab_c[...], lab_o[...], lab_t[0:1, :], lab_t[1:2, :]], axis=1).astype(F32)
    two_rows = jnp.concatenate([labels, jnp.zeros((1, 128), F32)], axis=0).astype(BF)
    cm[:, 2:4, 0:128] = jnp.broadcast_to(two_rows[None], (NQ, 2, 128))
    cm[:, 2:4, 128:256] = jnp.zeros((NQ, 2, 128), BF)
    reads[1].wait()
    for t in range(NQ):
        first = first_tile(t) * TILE
        size = min(TILE if t in SINGLE else WIDE, COEF - first)
        if size < WIDE:
            cm[t, 0:2, :] = jnp.zeros((2, WIDE), BF)
        cm[t, 0:2, 0:size] = rawr[0, :, first : first + size]

    reads[0].wait()

    for t in range(NQ):
        first = first_tile(t) * TILE
        size = min(TILE if t in SINGLE else WIDE, COEF - first)
        both = jnp.swapaxes(raw[:, :, first : first + size], 0, 1)
        for h in range(2):
            wide = min(TILE, size - h * TILE)
            if wide < TILE:
                xs[h, t] = jnp.zeros((PART, WIDE), BF)
            if wide > 0:
                for part in range(2):
                    xs[h, t, :, part * TILE : part * TILE + wide] = both[part, :, h * TILE : h * TILE + wide]
    pl.semaphore_wait(barrier, NQ - 1 + NZ - 1)

    mixed[0]()
    parts[0][0]()
    parts[1][0]()
    cb[pl.ds(q, 1)] = cm[pl.ds(q, 1)]

    @pl.when(jnp.logical_not(double))
    def _():
        xb[1] = jnp.zeros((NQ, PART, WIDE), BF)

    for h in range(2):
        xb[h, pl.ds(q, 1)] = xs[h, pl.ds(q, 1)]

    def features_of(turned):
        angle = turned[32:64] * (2.0 * math.pi / ORIENTS)
        low = -(40.0 + 1.5 * turned[64:96]) * (math.pi / 180.0)
        high = (40.0 + 1.5 * turned[96:128]) * (math.pi / 180.0)
        centre = low + high
        return jnp.sin(angle), jnp.cos(angle), jnp.cos(centre), jnp.sin(centre), jnp.cos(high - low)

    pad0[...] = jnp.broadcast_to(labels, (128, 128))
    own = features_of(pad0[...].T)

    def own_slice(s, power):
        for half in range(2):
            wedge = wedge_of(own, frequencies((first_tile(s) + half) * TILE))
            real = xs[half, s, :, 0:128].astype(F32)
            imag = xs[half, s, :, 128:256].astype(F32)
            power = power + wedge * (real * real + imag * imag)
        return power

    power = lax.fori_loop(0, NQ, own_slice, jnp.zeros((32, 128), F32), unroll=2)
    power = jnp.sum(power, axis=1, keepdims=True)

    mixed[1]()
    both = jnp.swapaxes(cb[:, 0:2, :], 0, 1)
    for h in range(2):
        for part in range(2):
            at = h * 256 + part * 128
            r1[:, at : at + 128] = both[part, :, h * 128 : h * 128 + 128]
    refsz[0]()
    rr[pl.ds(z, 1)] = r1[...][None]

    every = jnp.swapaxes(cb[:, 2:4, 0:128], 0, 1)[0].astype(F32)
    pad0[0:32, :] = every
    for k, feature in enumerate(features_of(pad0[...].T)):
        ft[k] = feature
    sub = lax.broadcasted_iota(jnp.int32, (32, 128), 0)
    cls = jnp.where(lax.broadcasted_iota(jnp.int32, (32, 128), 1) < 32, every, 0.0).astype(jnp.int32)
    in_plane = (((cls >> 3) & 7) * 32 + (cls >> 6) * 8 + (cls & 7)).astype(F32)
    chosen = in_plane
    for k in range(1, 4):
        chosen = jnp.where((sub & 3) == k, pltpu.roll(in_plane, 32 * k, 1), chosen)
    sel[...] = chosen
    class_row = lax.broadcasted_iota(jnp.int32, (CLASSES, 128), 0).astype(F32)
    for tile in range(8):
        row = jnp.sum(sel[4 * tile : 4 * tile + 4, :], axis=0, keepdims=True)
        oh[:, tile * 128 : tile * 128 + 128] = jnp.where(class_row == row, 1.0, 0.0).astype(BF)

    def features(s):
        index = jnp.full((32, 128), s, jnp.int32)
        return tuple(jnp.take_along_axis(ft[k], index, axis=1, mode="promise_in_bounds") for k in range(5))

    mine = [frequencies((first_tile(q) + h) * TILE) for h in range(2)]

    def weigh(s):
        feature = features(s)
        for half in range(2):
            wedge = wedge_of(feature, mine[half])
            where = (rows32(s), slice(half * 128, half * 128 + 128))
            wg[where] = wedge
            wlow[where] = wedge.astype(BF)
            wsq[where] = (wedge * wedge).astype(BF)

    over(0, NQ, weigh, unroll=2)

    contract = (((1,), (1,)), ((), ()))
    limits = (COEF, jnp.where(double, COEF, 0).astype(F32))
    valid = jnp.concatenate([jnp.where(mine[h][5] < limits[h], 1.0, 0.0) for h in range(2)], axis=1)
    valid = jnp.broadcast_to(valid, (8, WIDE)).astype(BF)
    total = lax.dot_general(valid, wlow[...], contract, preferred_element_type=F32)
    upper = total.astype(BF)
    rows = jnp.concatenate([jnp.ones((8, 1024), BF), upper, (total - upper.astype(F32)).astype(BF)], axis=0)
    found = lax.dot_general(rows, oh[...], contract, preferred_element_type=F32)
    s8[0:1] = found[0:1]
    s8[1:2] = found[8:9] + found[16:17]
    statz[0]()
    zs[pl.ds(z, 1)] = s8[...][None]

    db[...] = jnp.dot(oh[...], wsq[...], preferred_element_type=F32).astype(BF)

    def weigh_half(h):
        def weight(s):
            wedge = wg[rows32(s), h * 128 : h * 128 + 128]
            block = xb[h, s].astype(F32)
            wx[h, rows32(s), 0:128] = (wedge * block[:, 0:128]).astype(BF)
            wx[h, rows32(s), 128:256] = (wedge * block[:, 128:256]).astype(BF)

        over(0, NQ, weight, unroll=8)

    def half_sums(h):
        nb[h] = jnp.dot(oh[...], wx[h], preferred_element_type=F32).astype(BF)
        numz[h][0]()
        nr[h, pl.ds(z, 1)] = nb[h, rows32(z)][None]

    def give_back(k, swap, mine, theirs):
        swap.wait_recv()

        def add_core(t):
            sm[k, t] = (mine[t, c] + theirs[t]).astype(BF)

        over(0, 16, add_core, unroll=8)
        backs[k][0]()
        b1[k, pl.ds(chip, 1)] = sm[k, pl.ds(chip, 1)]

    parts[0][1]()
    weigh_half(0)
    half_sums(0)
    denz[0]()
    dr[pl.ds(z, 1)] = db[rows32(z)][None]

    refsz[1]()
    for plane in range(NZ):
        block = rr[plane].astype(F32)
        for k in range(NY):
            rf[k * 64 + plane * 8 : k * 64 + plane * 8 + 8, :] = block[8 * k : 8 * k + 8]
    for h in range(2):
        real = rf[:, h * 256 : h * 256 + 128]
        imag = rf[:, h * 256 + 128 : h * 256 + 256]
        rpow[:, h * 128 : h * 128 + 128] = (real * real + imag * imag).astype(BF)
    sbe[...] = lax.dot_general(wlow[...], rpow[...], contract, preferred_element_type=F32).reshape(16, 2, 32, CLASSES)
    swap_e.start()
    statz[1]()
    every = jnp.sum(zs[...], axis=0)
    here = every[1:2]
    tm[...] = jnp.where(z < 4, here[:, 0:128], here[:, 128:256])
    totals[0]()
    tmr[pl.ds(q, 1)] = tm[...][None]
    ids = lax.broadcasted_iota(jnp.int32, (CLASSES, CLASSES), 1)
    ids = ((ids >> 3) & 7) * 32 + (ids >> 6) * 8 + (ids & 7)
    order = jnp.where(lax.broadcasted_iota(jnp.int32, (CLASSES, CLASSES), 0) == ids, 1.0, 0.0).astype(BF)
    counts = jnp.broadcast_to(every[0:1], (8, CLASSES))
    upper = counts.astype(BF)
    rows = jnp.concatenate([upper, (counts - upper.astype(F32)).astype(BF)], axis=0)
    moved = jnp.dot(rows, order, preferred_element_type=F32)
    cv[...] = (moved[0:1] + moved[8:9]) * (CLASSES / PARTICLES)
    put_counts.start()

    give_back(0, swap_e, sbe, pbe)
    second_arrived()
    weigh_half(1)
    half_sums(1)


    part_sum = lax.dot_general(wx[0], rf[:, 0:256].astype(BF), contract, preferred_element_type=F32)
    part_sum = part_sum + lax.dot_general(wx[1], rf[:, 256:512].astype(BF), contract, preferred_element_type=F32)
    sbi[...] = part_sum.reshape(16, 2, 32, CLASSES)
    swap_i.start()
    give_back(1, swap_i, sbi, pbi)

    denz[1]()
    denom = jnp.sum(dr[...].astype(F32), axis=0)
    totals[1]()
    pad0[...] = jnp.broadcast_to(jnp.sum(tmr[...], axis=0), (128, 128)).T
    tail = pad0[pl.ds(pl.multiple_of((z % 4) * 32, 32), 32), 0:1]
    bottom = denom + TAU * (tail / COEF + 1.0)
    scale = 1.0 / bottom
    for h in range(2):
        numz[h][1]()
        top = jnp.sum(nr[h].astype(F32), axis=0)
        for part in range(2):
            lanes = slice(h * 128, h * 128 + 128)
            mb[:, part, lanes] = top[:, part * 128 : part * 128 + 128] * scale[:, lanes]
    means(0)

    backs[0][1]()
    energy = jnp.sum(b1[0].astype(F32), axis=0)
    backs[1][1]()
    inter = jnp.sum(b1[1].astype(F32), axis=0)
    sv[...] = inter / (
        math.sqrt(COEF) * jnp.sqrt((energy / COEF + EPS) * (power / COEF + EPS))
    )
    put_scores.start()
    means(1)
    for leaving in (put_counts, put_scores):
        leaving.wait()
    for group in (mixed, parts[0], totals, refsz, denz, *numz, statz, *backs):
        group[2]()
    swap_e.wait_send()
    swap_i.wait_send()
    second_sent()


def leave(score_in, mean_in, count_in, score_ref, mean_ref, count_ref):
    score_ref[...] = score_in[...]
    mean_ref[...] = mean_in[:, :, 0:COEF]
    count_ref[...] = count_in[...]


def body(particles, references, assignment, orientation, tilt_range):
    def v(*shape, dtype=F32):
        return pltpu.VMEM(shape, dtype)

    sem = pltpu.SemaphoreType.DMA
    vm = pl.BlockSpec(memory_space=pltpu.VMEM)
    hbm = pl.BlockSpec(memory_space=pltpu.HBM)
    def shapes(wide):
        return (
            jax.ShapeDtypeStruct((PART, CLASSES), F32),
            jax.ShapeDtypeStruct((1, 2, wide), F32),
            jax.ShapeDtypeStruct((1, CLASSES), F32),
        )

    outs = pl.pallas_call(
        kernel,
        out_shape=shapes(PADDED),
        in_specs=[hbm] * 5,
        out_specs=(hbm,) * 3,
        scratch_shapes=[
            v(PART, 2, COEF, dtype=BF), v(1, 2, COEF, dtype=BF),
            v(1, PART, dtype=jnp.int32), v(1, PART, dtype=jnp.int32), v(2, PART, dtype=jnp.int32),
            v(NQ, 4, WIDE, dtype=BF), v(NQ, 4, WIDE, dtype=BF),
            v(2, NQ, PART, WIDE, dtype=BF), v(2, NQ, PART, WIDE, dtype=BF),
            v(1, 128), v(NQ, 1, 128),
            v(32, 2 * WIDE, dtype=BF), v(NZ, 32, 2 * WIDE, dtype=BF),
            v(2, CLASSES, WIDE, dtype=BF), v(2, NZ, 32, WIDE, dtype=BF),
            v(CLASSES, WIDE, dtype=BF), v(NZ, 32, WIDE, dtype=BF),
            v(2, CLASSES), v(NZ, 2, CLASSES),
            v(128, 128), v(5, 32, 128), v(32, 128),
            v(CLASSES, 1024, dtype=BF), v(1024, WIDE), v(1024, WIDE, dtype=BF), v(1024, WIDE, dtype=BF),
            v(2, 1024, WIDE, dtype=BF), v(CLASSES, 2 * WIDE), v(CLASSES, WIDE, dtype=BF),
            v(16, 2, 32, CLASSES), v(16, 2, 32, CLASSES), v(16, 32, CLASSES), v(16, 32, CLASSES),
            v(2, 16, 32, CLASSES, dtype=BF), v(2, 16, 32, CLASSES, dtype=BF), v(NQ, 2, WIDE), v(PART, CLASSES), v(1, CLASSES),
        ] + [sem((2,)), sem((3,)), sem((3,))] + [sem((2,))] * 6 + [sem] * 16,
        compiler_params=pltpu.CompilerParams(
            collective_id=0, has_side_effects=True
        ),
    )(particles, references, assignment.T, orientation[None], tilt_range)
    scores, means, counts = pl.pallas_call(
        leave, out_shape=shapes(COEF), in_specs=[vm] * 3, out_specs=(vm,) * 3
    )(*outs)
    return scores, means, counts[0]


def solution(mesh):
    split = Mesh(mesh.devices.reshape(NY, NZ, NX, NC), DOM)
    placed = (P(DOM, None, None), P(DOM, None, None), P(DOM, None), P(DOM), P(None, DOM))
    return jax.shard_map(
        body,
        mesh=split,
        in_specs=placed,
        out_specs=(P(DOM, None), P(DOM, None, None), P()),
        check_vma=False,
    )
```
